256 devices in a mesh: det: 4 (over y), tm: 64 (over x, z, core).
Axes of the slice: x: 4, y: 4, z: 8, core: 2. Of those that a mesh axis runs over, the one named last changes fastest.
Arguments:
- detector_data: float32 [1024, 65536], P('det', 'tm'), may hold values from -250 to 250
- templates: bfloat16 [8, 16, 65536], P(None, None, 'tm'), may hold values from -5 to 5
- wafer_of: int32 [1024], P('det'), may hold values from 0 to 7, as said below
- knee_freq: float32 [1024], P(('det', 'tm')), may hold values from 0.1 to 5
- white_level: float32 [1024], P(('det', 'tm')), may hold values from 0.5 to 5
- tile_id: int32 [1024, 65536], P(('det', 'tm')), may hold values from 0 to 15
- pixel_id: int32 [1024, 65536], P(('det', 'tm')), may hold values from 0 to 127
- tile_order: int32 [16], replicated, may hold values from 0 to 15, each once
Outputs:
- fit_amps: float32 [16, 1024], P(None, 'det')
- weighted_data: bfloat16 [1024, 65536], P(('det', 'tm'))
- sky_map: float32 [2048], P('tm')
- weight_map: float32 [2048], P('tm')
The draws below stay inside these ranges and needn't reach their ends.
Inputs may be any that keep to these rules, and one draw needn't show every extreme that they name: `wafer_of`: the detectors of each aligned run of 128 share one wafer, and each wafer has exactly one such run.
All inputs are finite; a program needn't handle non-finite values.
Results may differ from the reference program's by a relative error of at most 0.0016.
Values sent between devices are 32-bit elements; how exact they have to be, the bound alone decides.
A program may use at most 64 MiB of HBM per device.

```python
import math
import jax
import jax.numpy as jnp
from jax import lax

SAMPLES = 65536
WAFERS = 8
MODES = 16
TILES = 16
PIX = 128
DETS = 1024


def shared_fields(key):
    base_key = jax.random.fold_in(key, 4242)
    subkeys = jax.random.split(base_key, 12)
    wafer_label = jax.random.permutation(subkeys[0], WAFERS).astype(jnp.int32)
    run_index = (jnp.arange(DETS, dtype=jnp.int32) // (DETS // WAFERS)).astype(jnp.int32)
    wafer_of = wafer_label[run_index]
    first_rank = jax.random.randint(subkeys[1], (DETS, SAMPLES), 0, TILES, dtype=jnp.int32)
    second_rank = jax.random.randint(subkeys[2], (DETS, SAMPLES), 0, TILES, dtype=jnp.int32)
    tile_label = jax.random.permutation(subkeys[3], TILES).astype(jnp.int32)
    tile_id = tile_label[jnp.minimum(first_rank, second_rank)]
    pixel_id = jax.random.randint(subkeys[4], (DETS, SAMPLES), 0, PIX, dtype=jnp.int32)
    return (wafer_of, tile_id, pixel_id, subkeys)


def template_values(subkeys):
    raw_values = jax.random.normal(subkeys[5], (WAFERS, MODES, SAMPLES), jnp.float32)
    return jnp.clip(raw_values, -5.0, 5.0)


def draw_templates(key, part):
    wafer_of, tile_id, pixel_id, subkeys = shared_fields(key)
    return template_values(subkeys).astype(jnp.bfloat16)


def draw_wafer_of(key, part):
    wafer_of, tile_id, pixel_id, subkeys = shared_fields(key)
    return wafer_of


def draw_tile_id(key, part):
    wafer_of, tile_id, pixel_id, subkeys = shared_fields(key)
    return tile_id


def draw_pixel_id(key, part):
    wafer_of, tile_id, pixel_id, subkeys = shared_fields(key)
    return pixel_id


def draw_detector_data(key, part):
    wafer_of, tile_id, pixel_id, subkeys = shared_fields(key)
    rounded = template_values(subkeys).astype(jnp.bfloat16).astype(jnp.float32)
    amplitude = jax.random.uniform(subkeys[7], (DETS, MODES), jnp.float32, -3.0, 3.0)
    wafer_hot = (wafer_of[:, None] == jnp.arange(WAFERS, dtype=jnp.int32)[None, :]).astype(jnp.float32)
    coefficients = (wafer_hot[:, :, None] * amplitude[:, None, :]).reshape(DETS, WAFERS * MODES)
    common_part = jnp.dot(coefficients, rounded.reshape(WAFERS * MODES, SAMPLES))
    sky_truth = jax.random.uniform(subkeys[8], (TILES, PIX), jnp.float32, -2.0, 2.0)
    sky_part = sky_truth[tile_id, pixel_id]
    noise_part = jnp.clip(jax.random.normal(subkeys[11], (DETS, SAMPLES), jnp.float32), -6.0, 6.0)
    return (common_part + sky_part + noise_part).astype(jnp.float32)


def level_of(key, extent, cuts, low, largest):
    factor_of = 1.0
    for position, blocks in cuts:
        steps = jax.random.uniform(jax.random.fold_in(jax.random.fold_in(key, 6), position), (blocks,), jnp.float32, low / len(cuts), largest / len(cuts))
        factor_of = factor_of * jnp.repeat(jnp.exp(steps), extent[position] // blocks).reshape((-1,) + (1,) * (len(extent) - 1 - position))
    return factor_of


def setup_inputs(seed: int = 0) -> dict:
    seeds = jax.random.split(jax.random.key(seed), 9)
    detector_data = draw_detector_data(jax.random.fold_in(seeds[8], 71), 0)
    templates = draw_templates(jax.random.fold_in(seeds[8], 71), 0)
    wafer_of = draw_wafer_of(jax.random.fold_in(seeds[8], 71), 0)
    knee_freq = jnp.clip(jnp.exp(math.log(5.0) - 3.912023 * jax.random.uniform(seeds[3], (DETS,), jnp.float32) ** level_of(seeds[3], (DETS,), ((0, 256),), -0.2, 0.2)), 0.1, 5.0)
    white_level = jnp.clip(jnp.exp(math.log(5.0) - 2.3025851 * jax.random.uniform(seeds[4], (DETS,), jnp.float32) ** level_of(seeds[4], (DETS,), ((0, 256),), -0.2, 0.2)), 0.5, 5.0)
    tile_id = draw_tile_id(jax.random.fold_in(seeds[8], 71), 0)
    pixel_id = draw_pixel_id(jax.random.fold_in(seeds[8], 71), 0)
    tile_order = jax.random.permutation(seeds[7], TILES).astype(jnp.int32)
    return dict(detector_data=detector_data, templates=templates, wafer_of=wafer_of, knee_freq=knee_freq, white_level=white_level, tile_id=tile_id, pixel_id=pixel_id, tile_order=tile_order)


precise = lax.Precision.HIGHEST
sample_rate = 200.0


def invert_blocks(matrices):
    dimension = matrices.shape[-1]
    identity = jnp.broadcast_to(jnp.eye(dimension, dtype=matrices.dtype), matrices.shape)
    joined = jnp.concatenate([matrices, identity], axis=-1)
    for column in range(dimension):
        pivot_row = joined[:, column, :] / joined[:, column, column][:, None]
        factor = joined[:, :, column]
        joined = joined - factor[:, :, None] * pivot_row[:, None, :]
        joined = joined.at[:, column, :].set(pivot_row)
    return joined[:, :, dimension:]


def spectral_weight(frequency, knee_rows, white_rows):
    squared = frequency * frequency
    return squared[None, :] / (white_rows[:, None] * (squared[None, :] + knee_rows[:, None] ** 2))


def reference(detector_data, templates, wafer_of, knee_freq, white_level, tile_id, pixel_id, tile_order):
    wafer_count = templates.shape[0]
    mode_count = templates.shape[1]
    full_length = templates.shape[2]
    detector_count = detector_data.shape[0]
    wide_templates = templates.astype(jnp.float32)
    flat_templates = wide_templates.reshape(wafer_count * mode_count, full_length)
    gram_matrix = jnp.einsum('wkt,wjt->wkj', wide_templates, wide_templates, precision=precise)
    inverse_gram = invert_blocks(gram_matrix)
    block_rows = math.gcd(detector_count, 64)
    block_count = detector_count // block_rows
    wafer_ramp = jnp.arange(wafer_count, dtype=jnp.int32)
    bin_index = jnp.arange(full_length // 2 + 1).astype(jnp.float32)
    frequency = bin_index * (sample_rate / full_length)
    cell_total = TILES * PIX

    def one_block(totals, inputs):
        data_rows, wafer_rows, knee_rows, white_rows, tile_rows, pixel_rows = inputs
        wafer_hot = (wafer_rows[None, :] == wafer_ramp[:, None]).astype(jnp.float32)
        projected = jnp.einsum('ct,bt->cb', flat_templates, data_rows, precision=precise)
        projected = projected.reshape(wafer_count, mode_count, block_rows)
        solved = jnp.einsum('wkj,wjb->wkb', inverse_gram, projected, precision=precise)
        amps_rows = jnp.einsum('wkb,wb->kb', solved, wafer_hot, precision=precise)
        coefficients = (wafer_hot[:, None, :] * amps_rows[None, :, :]).reshape(wafer_count * mode_count, block_rows)
        fitted = jnp.einsum('cb,ct->bt', coefficients, flat_templates, precision=precise)
        residual = data_rows - fitted
        spectrum = jnp.fft.rfft(residual, axis=-1)
        filtered = jnp.fft.irfft(spectrum * spectral_weight(frequency, knee_rows, white_rows), n=full_length, axis=-1)
        weighted_rows = filtered.astype(jnp.float32).astype(jnp.bfloat16)
        inverse_white = (1.0 / white_rows).astype(jnp.bfloat16)
        cell_rows = (tile_rows * PIX + pixel_rows).reshape(-1).astype(jnp.int32)
        values = lax.optimization_barrier(weighted_rows).astype(jnp.float32).reshape(-1)
        white_wide = lax.optimization_barrier(inverse_white).astype(jnp.float32)
        weights = jnp.broadcast_to(white_wide[:, None], tile_rows.shape).reshape(-1)
        sky_part = jax.ops.segment_sum(values, cell_rows, num_segments=cell_total)
        weight_part = jax.ops.segment_sum(weights, cell_rows, num_segments=cell_total)
        return (totals[0] + sky_part, totals[1] + weight_part), (amps_rows, weighted_rows)

    inputs = (
        detector_data.reshape(block_count, block_rows, full_length),
        wafer_of.reshape(block_count, block_rows),
        knee_freq.reshape(block_count, block_rows),
        white_level.reshape(block_count, block_rows),
        tile_id.reshape(block_count, block_rows, full_length),
        pixel_id.reshape(block_count, block_rows, full_length),
    )
    start_totals = (jnp.zeros((cell_total,), jnp.float32), jnp.zeros((cell_total,), jnp.float32))
    totals, outputs = lax.scan(one_block, start_totals, inputs)
    amps_blocks, weighted_blocks = outputs
    fit_amps = jnp.transpose(amps_blocks, (1, 0, 2)).reshape(mode_count, detector_count)
    weighted_data = weighted_blocks.reshape(detector_count, full_length)
    scale = float(TILES * PIX) / float(detector_count * full_length)
    sky_map = totals[0].reshape(TILES, PIX)[tile_order].reshape(-1) * scale
    weight_map = totals[1].reshape(TILES, PIX)[tile_order].reshape(-1) * scale
    return fit_amps, weighted_data, sky_map, weight_map
```

```python
import functools
import math

import jax
import jax.numpy as jnp
import numpy as np
from jax import lax
from jax.experimental import pallas as pl
from jax.experimental.pallas import tpu as pltpu
from jax.sharding import PartitionSpec as P

PIX = 128
MODES = 16
LANES = 128
SIDE = 256
HALF = SIDE // 2
ROWS = HALF + 8
sample_rate = 200.0
f32 = jnp.float32
bf16 = jnp.bfloat16
MESH = pl.DeviceIdType.MESH
NT = (((1,), (1,)), ((), ()))
NN = (((1,), (0,)), ((), ()))


def mm(a, b, dims=NN):
    return lax.dot_general(a, b, dims, preferred_element_type=f32)


def split2(x):
    high = x.astype(bf16)
    low = (x - high.astype(f32)).astype(bf16)
    return high, low


def split3(x):
    high = x.astype(bf16)
    rest = x - high.astype(f32)
    mid = rest.astype(bf16)
    low = (rest - mid.astype(f32)).astype(bf16)
    return high, mid, low


def fit_kernel(
    sizes, wafer_ref, data_ref, templates_ref, amps_ref, out_ref,
    parts, from_core, x_slots, z_slots, both, core_send, core_recv, x_send, x_recv, z_send, z_recv
):
    x_size, z_size = sizes
    tm = lax.axis_index("tm")
    core = tm % 2
    z = (tm // 2) % z_size
    x = tm // (2 * z_size)

    def index_of(x_at, z_at, core_at):
        return (x_at * z_size + z_at) * 2 + core_at

    other = index_of(x, z, 1 - core)
    x_peers = [index_of((x + k) % x_size, z, core) for k in range(1, x_size)]
    z_peers = [index_of(x, (z + k) % z_size, core) for k in range(1, z_size)]
    peers = [other] + x_peers + z_peers
    barrier = pltpu.get_barrier_semaphore()
    for peer in peers:
        pl.semaphore_signal(barrier, inc=1, device_id={"tm": peer}, device_id_type=MESH)

    run = data_ref.shape[0] // 2
    shapes = []
    for w in range(2):
        shape = templates_ref[wafer_ref[w * run]]
        shapes.append(shape)
        high, mid, low = split3(data_ref[w * run : (w + 1) * run, :])
        projected = mm(shape, high, NT) + mm(shape, mid, NT) + mm(shape, low, NT)
        gram = mm(shape, shape, NT)
        parts[w, 0:MODES, :] = projected
        pad = jnp.zeros((8, LANES - 2 * MODES), f32)
        parts[w, MODES : MODES + 8, :] = jnp.concatenate([gram[0:8], gram[8:16], pad], axis=1)

    pl.semaphore_wait(barrier, len(peers))
    copy = pltpu.make_async_remote_copy(
        src_ref=parts.at[1 - core], dst_ref=from_core, send_sem=core_send.at[0], recv_sem=core_recv.at[0],
        device_id={"tm": other}, device_id_type=MESH,
    )
    copy.start()
    copy.wait()
    mine = parts[core] + from_core[...]

    def exchange(mine, slots, place, peers, send_sem, recv_sem):
        slots[place] = mine
        copies = []
        for k, peer in enumerate(peers):
            copy = pltpu.make_async_remote_copy(
                src_ref=slots.at[place], dst_ref=slots.at[place], send_sem=send_sem.at[k], recv_sem=recv_sem.at[k],
                device_id={"tm": peer}, device_id_type=MESH,
            )
            copy.start()
            copies.append(copy)
        for copy in copies:
            copy.wait()
        total = slots[0]
        for k in range(1, len(peers) + 1):
            total = total + slots[k]
        return total

    mine = exchange(mine, x_slots, x, x_peers, x_send, x_recv)
    mine = exchange(mine, z_slots, z, z_peers, z_send, z_recv)
    both[core] = mine
    copy = pltpu.make_async_remote_copy(
        src_ref=both.at[core], dst_ref=both.at[core], send_sem=core_send.at[1], recv_sem=core_recv.at[1],
        device_id={"tm": other}, device_id_type=MESH,
    )
    copy.start()
    copy.wait()

    row = lax.broadcasted_iota(jnp.int32, (1, MODES, LANES), 1)
    for w in range(2):
        packed = both[w, MODES : MODES + 8, :]
        columns = []
        for k in range(MODES):
            top = jnp.broadcast_to(packed[:, k : k + 1], (8, LANES))
            low = jnp.broadcast_to(packed[:, MODES + k : MODES + k + 1], (8, LANES))
            columns.append(jnp.concatenate([top, low], axis=0))
        columns.append(both[w, 0:MODES, :])
        joined = jnp.stack(columns, axis=0)
        for c in range(MODES):
            factor = joined[0:1]
            pivot_row = joined[1:, c : c + 1, :] / factor[:, c : c + 1, :]
            joined = jnp.where(row == c, pivot_row, joined[1:] - factor * pivot_row)
        amps = joined[0]
        amps_ref[:, w * run : (w + 1) * run] = amps
        high, mid, low = split3(amps)
        left = jnp.concatenate([high, mid, low], axis=0)
        right = jnp.concatenate([shapes[w]] * 3, axis=0)
        fitted = lax.dot_general(left, right, (((0,), (0,)), ((), ())), preferred_element_type=f32)
        residual = data_ref[w * run : (w + 1) * run, :] - fitted
        tiles = residual.shape[1] // LANES
        for l in range(tiles):
            out_ref[pl.ds(w * run * tiles + l, run, stride=tiles), :] = residual[:, l * LANES : (l + 1) * LANES]


def fit(mesh, detector_data, templates, wafer_of):
    rows, local = detector_data.shape
    x_size, z_size = 4, 8
    part = (MODES + 8, LANES)
    return pl.pallas_call(
        functools.partial(fit_kernel, (x_size, z_size)),
        out_shape=(
            jax.ShapeDtypeStruct((MODES, rows), f32),
            jax.ShapeDtypeStruct((rows * local // LANES, LANES), f32),
        ),
        in_specs=[
            pl.BlockSpec(memory_space=pltpu.SMEM),
            pl.BlockSpec(memory_space=pltpu.VMEM),
            pl.BlockSpec(memory_space=pltpu.VMEM),
        ],
        out_specs=[pl.BlockSpec(memory_space=pltpu.VMEM)] * 2,
        scratch_shapes=[
            pltpu.VMEM((2,) + part, f32),
            pltpu.VMEM(part, f32),
            pltpu.VMEM((x_size,) + part, f32),
            pltpu.VMEM((z_size,) + part, f32),
            pltpu.VMEM((2,) + part, f32),
            pltpu.SemaphoreType.DMA((2,)),
            pltpu.SemaphoreType.DMA((2,)),
            pltpu.SemaphoreType.DMA((x_size - 1,)),
            pltpu.SemaphoreType.DMA((x_size - 1,)),
            pltpu.SemaphoreType.DMA((z_size - 1,)),
            pltpu.SemaphoreType.DMA((z_size - 1,)),
        ],
        compiler_params=pltpu.CompilerParams(collective_id=0, has_side_effects=True),
        name="fit",
    )(wafer_of, detector_data, templates)


CHUNK = 2048


def cell_hots(tile_ref, pixel_ref, start, values=None):
    span = pl.ds(pl.multiple_of(start, CHUNK), CHUNK)
    tiles = tile_ref[:, span]
    pixels = pixel_ref[:, span]
    left_id = (tiles + 16 * (pixels >> 6)).astype(f32).astype(bf16)
    right_id = (pixels & 63).astype(f32).astype(bf16)
    return left_id, right_id


def counts_kernel(tile_ref, pixel_ref, white_ref, out_ref):
    dets, samples = tile_ref.shape
    left_ramp = lax.broadcasted_iota(jnp.int32, (32, CHUNK), 0).astype(f32).astype(bf16)
    right_ramp = lax.broadcasted_iota(jnp.int32, (64, CHUNK), 0).astype(f32).astype(bf16)
    one, zero = jnp.ones((), bf16), jnp.zeros((), bf16)

    def step(turn, totals):
        left_id, right_id = cell_hots(tile_ref, pixel_ref, turn * CHUNK)
        fresh = []
        for d in range(dets):
            left = jnp.where(left_id[d : d + 1] == left_ramp, one, zero)
            right = jnp.where(right_id[d : d + 1] == right_ramp, one, zero)
            fresh.append(totals[d] + mm(left, right, NT))
        return tuple(fresh)

    totals = lax.fori_loop(0, samples // CHUNK, step, (jnp.zeros((32, 64), f32),) * dets)
    total = jnp.zeros((32, 64), f32)
    for d in range(dets):
        inverse = (jnp.ones((1, 64), f32) / jnp.full((1, 64), white_ref[d], f32)).astype(bf16).astype(f32)
        total = total + totals[d] * inverse
    out_ref[...] = jnp.concatenate([total[0:16], total[16:32]], axis=1)


def counts(tile_id, pixel_id, white_level):
    vmem = pl.BlockSpec(memory_space=pltpu.VMEM)
    return pl.pallas_call(
        counts_kernel,
        out_shape=jax.ShapeDtypeStruct((16, LANES), f32),
        in_specs=[vmem, vmem, pl.BlockSpec(memory_space=pltpu.SMEM)],
        out_specs=vmem,
        cost_estimate=pl.CostEstimate(flops=10**10, bytes_accessed=2**21, transcendentals=0),
        name="counts",
    )(tile_id, pixel_id, white_level)


def tables(chunks):
    full = SIDE * SIDE
    per = SIDE // chunks
    ramp = np.arange(SIDE)
    order = np.array([per * s + j for j in range(per) for s in range(chunks)])
    angle = 2.0 * np.pi / SIDE * (np.outer(ramp, ramp) % SIDE)
    cos, sin = np.cos(angle), np.sin(angle)
    first = np.concatenate([cos[:HALF], -sin[:HALF]], axis=0)
    first[HALF] = cos[HALF]
    second = np.block([[cos, -sin], [sin, cos]])
    weight = np.full((HALF,), 2.0)
    weight[0] = 1.0
    last = np.concatenate([cos[:, :HALF] * weight, -sin[:, :HALF] * weight], axis=1)
    last[:, HALF] = cos[:, HALF]
    k = np.arange(ROWS)
    turn = 2.0 * np.pi / full * np.outer(k, ramp)
    valid = (k <= HALF)[:, None]
    turn_cos, turn_sin = np.cos(turn) * valid, np.sin(turn) * valid
    bins = k[:, None] + SIDE * ramp[None, :]
    folded = np.minimum(bins, full - bins).astype(np.float32)
    frequency = folded * np.float32(sample_rate / full)
    squared = np.where(valid, frequency * frequency, np.float32(0)).astype(np.float32)

    def halves(a):
        a = a.astype(np.float32)
        high = a.astype(jnp.bfloat16)
        return high, (a - high.astype(np.float32)).astype(jnp.bfloat16)

    return (
        *halves(first[:, order]),
        *halves(second),
        *halves(last / full),
        turn_cos.astype(np.float32),
        turn_sin.astype(np.float32),
        squared,
    )


def three(left, right, dims=NN):
    return mm(left[0], right[0], dims) + mm(left[0], right[1], dims) + mm(left[1], right[0], dims)


def filter_kernel(
    scale, knee_ref, white_ref, order_ref, data_ref, tile_ref, pixel_ref, weight_ref,
    first_high, first_low, second_high, second_low, last_high, last_low, turn_cos, turn_sin, squared_ref,
    weighted_ref, maps_ref,
    flat, comb, tm_slots, det_slots, tm_send, tm_recv, det_send, det_recv
):
    dets = tile_ref.shape[0]
    samples = tile_ref.shape[1]
    owners = tm_slots.shape[0]
    det_size = det_slots.shape[0]
    tm = lax.axis_index("tm")
    det = lax.axis_index("det")
    barrier = pltpu.get_barrier_semaphore()

    def greet(k, carry):
        pl.semaphore_signal(barrier, inc=1, device_id={"tm": (tm + k) % owners}, device_id_type=MESH)
        return carry

    lax.fori_loop(1, owners, greet, 0)
    for k in range(1, det_size):
        pl.semaphore_signal(barrier, inc=1, device_id={"det": (det + k) % det_size}, device_id_type=MESH)

    chunks = owners
    per = SIDE // chunks
    tiles = SIDE // LANES
    block = per * tiles
    for d in range(dets):
        rows = []
        for j in range(per):
            rows.append(
                jnp.concatenate(
                    [
                        data_ref[pl.ds(d * block + j * tiles + h, chunks, stride=dets * block), :]
                        for h in range(tiles)
                    ],
                    axis=1,
                )
            )
        signal = jnp.concatenate(rows, axis=0)
        spectrum = three((first_high[...], first_low[...]), split2(signal))
        real_y, imag_y, tail = spectrum[0:HALF], spectrum[HALF:], spectrum[HALF : HALF + 8]
        first_row = lax.broadcasted_iota(jnp.int32, (HALF, SIDE), 0) == 0
        imag_y = jnp.where(first_row, 0.0, imag_y)
        cos_main, sin_main = turn_cos[0:HALF, :], turn_sin[0:HALF, :]
        cos_tail, sin_tail = turn_cos[HALF:, :], turn_sin[HALF:, :]
        real_z = jnp.concatenate([real_y * cos_main + imag_y * sin_main, tail * cos_tail], axis=0)
        imag_z = jnp.concatenate([imag_y * cos_main - real_y * sin_main, -tail * sin_tail], axis=0)
        bins = three(
            split2(jnp.concatenate([real_z, imag_z], axis=1)), (second_high[...], second_low[...])
        )
        squared = squared_ref[...]
        knee = knee_ref[d]
        gain = squared / (white_ref[d] * (squared + knee * knee))
        bins = bins * jnp.concatenate([gain, gain], axis=1)
        back = three(split2(bins), (second_high[...], second_low[...]), NT)
        real_u, imag_u = back[:, 0:SIDE], back[:, SIDE:]
        real_w = real_u[0:HALF] * cos_main - imag_u[0:HALF] * sin_main
        imag_w = real_u[0:HALF] * sin_main + imag_u[0:HALF] * cos_main
        tail_w = (real_u[HALF:] * cos_tail - imag_u[HALF:] * sin_tail)[0:1]
        imag_w = jnp.where(first_row, jnp.broadcast_to(tail_w, (HALF, SIDE)), imag_w)
        joined = jnp.concatenate([real_w, imag_w], axis=0)
        output = three((last_high[...], last_low[...]), split2(joined))
        for h in range(tiles):
            flat[pl.ds(h * dets + d, SIDE, stride=tiles * dets), :] = output[:, h * LANES : (h + 1) * LANES]
    weighted_ref[...] = flat[...].astype(bf16)

    left_ramp = lax.broadcasted_iota(jnp.int32, (32, CHUNK), 0).astype(f32).astype(bf16)
    right_ramp = lax.broadcasted_iota(jnp.int32, (64, CHUNK), 0).astype(f32).astype(bf16)
    one, zero = jnp.ones((), bf16), jnp.zeros((), bf16)

    def step(turn, total):
        left_id, right_id = cell_hots(tile_ref, pixel_ref, turn * CHUNK)
        width = CHUNK // LANES * dets
        values = flat[pl.ds(pl.multiple_of(turn * width, width), width), :].astype(bf16)
        for d in range(dets):
            value = jnp.concatenate(
                [values[l * dets + d : l * dets + d + 1, :] for l in range(CHUNK // LANES)], axis=1
            )
            left = jnp.where(left_id[d : d + 1] == left_ramp, value, zero)
            right = jnp.where(right_id[d : d + 1] == right_ramp, one, zero)
            total = total + mm(left, right, NT)
        return total

    total = lax.fori_loop(0, samples // CHUNK, step, jnp.zeros((32, 64), f32))
    comb[0] = jnp.concatenate([total[0:16], total[16:32]], axis=1)
    comb[1] = weight_ref[...]

    ordered = tm_slots.shape
    del ordered
    for r in range(16):
        tile = order_ref[r]
        maps_ref[r, 0:1, :] = comb[0, pl.ds(tile, 1), :]
        maps_ref[r, 1:2, :] = comb[1, pl.ds(tile, 1), :]
    share = owners // 16

    pl.semaphore_wait(barrier, owners - 1 + det_size - 1)

    def send(k, carry):
        peer = (tm + k) % owners
        pltpu.make_async_remote_copy(
            src_ref=maps_ref.at[peer // share], dst_ref=tm_slots.at[tm], send_sem=tm_send, recv_sem=tm_recv,
            device_id={"tm": peer}, device_id_type=MESH,
        ).start()
        return carry

    lax.fori_loop(1, owners, send, 0)
    tm_slots[tm] = maps_ref[tm // share]
    everything = pltpu.make_async_remote_copy(
        src_ref=tm_slots.at[pl.ds(0, owners - 1)], dst_ref=tm_slots.at[pl.ds(0, owners - 1)],
        send_sem=tm_send, recv_sem=tm_recv, device_id={"tm": (tm + 1) % owners}, device_id_type=MESH,
    )
    everything.wait()
    det_slots[det] = jnp.sum(tm_slots[...], axis=0)
    copies = []
    for k in range(1, det_size):
        copy = pltpu.make_async_remote_copy(
            src_ref=det_slots.at[det], dst_ref=det_slots.at[det], send_sem=det_send.at[k - 1],
            recv_sem=det_recv.at[k - 1], device_id={"det": (det + k) % det_size}, device_id_type=MESH,
        )
        copy.start()
        copies.append(copy)
    for copy in copies:
        copy.wait()
    total = det_slots[0]
    for k in range(1, det_size):
        total = total + det_slots[k]
    maps_ref[0] = total * scale


def weigh(scale, det_size, owners, knee_freq, white_level, tile_order, data, tile_id, pixel_id, weight_part):
    dets, samples = tile_id.shape
    vmem = pl.BlockSpec(memory_space=pltpu.VMEM)
    smem = pl.BlockSpec(memory_space=pltpu.SMEM)
    factors = tables(owners)
    return pl.pallas_call(
        functools.partial(filter_kernel, scale),
        out_shape=(
            jax.ShapeDtypeStruct((dets * samples // LANES, LANES), bf16),
            jax.ShapeDtypeStruct((16, 2, LANES), f32),
        ),
        in_specs=[smem] * 3 + [vmem] * (4 + len(factors)),
        out_specs=[vmem] * 2,
        scratch_shapes=[
            pltpu.VMEM((dets * samples // LANES, LANES), f32),
            pltpu.VMEM((2, 16, LANES), f32),
            pltpu.VMEM((owners, 2, LANES), f32),
            pltpu.VMEM((det_size, 2, LANES), f32),
            pltpu.SemaphoreType.DMA,
            pltpu.SemaphoreType.DMA,
            pltpu.SemaphoreType.DMA((det_size - 1,)),
            pltpu.SemaphoreType.DMA((det_size - 1,)),
        ],
        compiler_params=pltpu.CompilerParams(collective_id=1, has_side_effects=True),
        name="weigh",
    )(knee_freq, white_level, tile_order, data, tile_id, pixel_id, weight_part, *factors)


def shards(
    mesh, detector_data, templates, wafer_of, knee_freq, white_level, tile_id, pixel_id, tile_order
):
    owners = mesh.shape["tm"]
    det_size = mesh.shape["det"]
    dets, samples = tile_id.shape
    fit_amps, residual = fit(mesh, detector_data, templates, wafer_of)
    rows = residual.shape[0] // owners
    moved = lax.all_to_all(residual.reshape(owners, rows, LANES), "tm", split_axis=0, concat_axis=0, tiled=True)
    moved = moved.reshape(owners * rows, LANES)
    weight_part = counts(tile_id, pixel_id, white_level)
    cells = 16 * PIX
    scale = float(cells) / float(dets * owners * det_size * samples)
    weighted, maps = weigh(
        scale, det_size, owners, knee_freq, white_level, tile_order, moved, tile_id, pixel_id, weight_part
    )
    weighted = weighted.reshape(samples // LANES, dets, LANES).transpose(1, 0, 2).reshape(dets, samples)
    share = cells // owners
    start = (lax.axis_index("tm") % (PIX // share)) * share
    own = lax.dynamic_slice(maps[0], (0, start), (2, share))
    return (fit_amps, weighted, own[0], own[1])


def solution(mesh):
    in_specs = (
        P("det", "tm"),
        P(None, None, "tm"),
        P("det"),
        P(("det", "tm")),
        P(("det", "tm")),
        P(("det", "tm"), None),
        P(("det", "tm"), None),
        P(),
    )
    out_specs = (P(None, "det"), P(("det", "tm"), None), P("tm"), P("tm"))
    return jax.shard_map(
        functools.partial(shards, mesh), mesh=mesh, in_specs=in_specs, out_specs=out_specs, check_vma=False
    )
```

```python
import functools
import math

import jax
import jax.numpy as jnp
import numpy as np
from jax import lax
from jax.experimental import pallas as pl
from jax.experimental.pallas import tpu as pltpu
from jax.sharding import PartitionSpec as P

PIX = 128
MODES = 16
LANES = 128
SIDE = 256
HALF = SIDE // 2
ROWS = HALF + 8
sample_rate = 200.0
f32 = jnp.float32
bf16 = jnp.bfloat16
MESH = pl.DeviceIdType.MESH
NT = (((1,), (1,)), ((), ()))
NN = (((1,), (0,)), ((), ()))


def mm(a, b, dims=NN):
    return lax.dot_general(a, b, dims, preferred_element_type=f32)


def split2(x):
    high = x.astype(bf16)
    low = (x - high.astype(f32)).astype(bf16)
    return high, low


def split3(x):
    high = x.astype(bf16)
    rest = x - high.astype(f32)
    mid = rest.astype(bf16)
    low = (rest - mid.astype(f32)).astype(bf16)
    return high, mid, low


def tables(chunks):
    full = SIDE * SIDE
    per = SIDE // chunks
    ramp = np.arange(SIDE)
    order = np.array([per * s + j for j in range(per) for s in range(chunks)])
    angle = 2.0 * np.pi / SIDE * (np.outer(ramp, ramp) % SIDE)
    cos, sin = np.cos(angle), np.sin(angle)
    first = np.concatenate([cos[:HALF], -sin[:HALF]], axis=0)
    first[HALF] = cos[HALF]
    second = np.block([[cos, -sin], [sin, cos]])
    weight = np.full((HALF,), 2.0)
    weight[0] = 1.0
    last = np.concatenate([cos[:, :HALF] * weight, -sin[:, :HALF] * weight], axis=1)
    last[:, HALF] = cos[:, HALF]
    k = np.arange(ROWS)
    turn = 2.0 * np.pi / full * np.outer(k, ramp)
    valid = (k <= HALF)[:, None]
    turn_cos, turn_sin = np.cos(turn) * valid, np.sin(turn) * valid
    bins = k[:, None] + SIDE * ramp[None, :]
    folded = np.minimum(bins, full - bins).astype(np.float32)
    frequency = folded * np.float32(sample_rate / full)
    squared = np.where(valid, frequency * frequency, np.float32(0)).astype(np.float32)

    def halves(a):
        a = a.astype(np.float32)
        high = a.astype(jnp.bfloat16)
        return high, (a - high.astype(np.float32)).astype(jnp.bfloat16)

    return (
        *halves(first[:, order]),
        *halves(second),
        *halves(last / full),
        turn_cos.astype(np.float32),
        turn_sin.astype(np.float32),
        squared,
    )


def three(left, right, dims=NN):
    return mm(left[0], right[0], dims) + mm(left[0], right[1], dims) + mm(left[1], right[0], dims)


CHUNK = 8192
f8 = jnp.float8_e4m3fn


def whole_kernel(
    sizes, scale, wafer_ref, knee_ref, white_ref, order_ref, data_ref, templates_ref, *refs
):
    x_size, z_size, det_size = sizes
    stored, refs = refs[:11], refs[11:]
    amps_ref, flat, maps_ref = refs[:3]
    held, refs = refs[3:14], refs[14:]
    (
        fetch_sem, left_ids, right_ids, parts, from_core, x_slots, z_slots, both, sent, got, comb, rows_out,
        tm_slots, det_slots, core_send, core_recv, x_send, x_recv, z_send, z_recv, move_send, move_recv,
        tm_send, tm_recv, det_send, det_recv,
    ) = refs
    tile_ref, pixel_ref = held[:2]
    first_high, first_low, second_high, second_low, last_high, last_low, turn_cos, turn_sin, squared_ref = held[2:]
    dets, samples = tile_ref.shape
    owners = x_size * z_size * 2
    tm = lax.axis_index("tm")
    det = lax.axis_index("det")
    core = tm % 2
    z = (tm // 2) % z_size
    x = tm // (2 * z_size)

    def index_of(x_at, z_at, core_at):
        return (x_at * z_size + z_at) * 2 + core_at

    other = index_of(x, z, 1 - core)
    x_peers = [index_of((x + k) % x_size, z, core) for k in range(1, x_size)]
    z_peers = [index_of(x, (z + k) % z_size, core) for k in range(1, z_size)]
    peers = [other] + x_peers + z_peers
    barrier = pltpu.get_barrier_semaphore()
    for peer in peers:
        pl.semaphore_signal(barrier, inc=1, device_id={"tm": peer}, device_id_type=MESH)
    for k in range(1, det_size):
        pl.semaphore_signal(barrier, inc=1, device_id={"det": (det + k) % det_size}, device_id_type=MESH)
    fetches = [
        pltpu.make_async_copy(stored[k], held[k], fetch_sem.at[k]) for k in range(len(stored))
    ]
    for fetch in fetches:
        fetch.start()

    run = data_ref.shape[0] // 2
    shapes = []
    for w in range(2):
        shape = templates_ref[wafer_ref[w * run]]
        shapes.append(shape)
        high, mid, low = split3(data_ref[w * run : (w + 1) * run, :])
        projected = mm(shape, high, NT) + mm(shape, mid, NT) + mm(shape, low, NT)
        gram = mm(shape, shape, NT)
        parts[w, 0:MODES, :] = projected
        pad = jnp.zeros((8, LANES - 2 * MODES), f32)
        parts[w, MODES : MODES + 8, :] = jnp.concatenate([gram[0:8], gram[8:16], pad], axis=1)

    pl.semaphore_wait(barrier, len(peers) + det_size - 1)
    copy = pltpu.make_async_remote_copy(
        src_ref=parts.at[1 - core], dst_ref=from_core, send_sem=core_send.at[0], recv_sem=core_recv.at[0],
        device_id={"tm": other}, device_id_type=MESH,
    )
    copy.start()

    def ids(turn, carry):
        span = pl.ds(pl.multiple_of(turn * CHUNK, CHUNK), CHUNK)
        tiles = tile_ref[:, span]
        pixels = pixel_ref[:, span]
        left_ids[:, span] = (tiles + 16 * (pixels >> 6)).astype(f32)
        right_ids[:, span] = (pixels & 63).astype(f32)
        return carry

    for fetch in fetches[:2]:
        fetch.wait()
    lax.fori_loop(0, samples // CHUNK, ids, 0)
    copy.wait()
    mine = parts[core] + from_core[...]

    one, zero = jnp.ones((), bf16), jnp.zeros((), bf16)

    def ramp(rows):
        return lax.broadcasted_iota(jnp.int32, (rows, CHUNK), 0).astype(f32).astype(bf16)

    def binned(d, total, value_of):
        def step(turn, total):
            span = pl.ds(pl.multiple_of(turn * CHUNK, CHUNK), CHUNK)
            left_id = left_ids[pl.ds(d, 1), span].astype(bf16)
            right_id = right_ids[pl.ds(d, 1), span].astype(bf16)
            left = jnp.where(left_id == ramp(32), value_of(turn), zero)
            right = jnp.where(right_id == ramp(64), one, zero).astype(f8)
            return total + mm(left, right, NT)

        return lax.fori_loop(0, samples // CHUNK, step, total)

    def count(d, total):
        inverse = (jnp.ones((1, 64), f32) / jnp.full((1, 64), white_ref[d], f32)).astype(bf16).astype(f32)
        return total + binned(d, jnp.zeros((32, 64), f32), lambda turn: one) * inverse

    def exchange(mine, slots, place, peers, send_sem, recv_sem, meanwhile):
        slots[place] = mine
        copies = []
        for k, peer in enumerate(peers):
            copy = pltpu.make_async_remote_copy(
                src_ref=slots.at[place], dst_ref=slots.at[place], send_sem=send_sem.at[k], recv_sem=recv_sem.at[k],
                device_id={"tm": peer}, device_id_type=MESH,
            )
            copy.start()
            copies.append(copy)
        result = meanwhile()
        for copy in copies:
            copy.wait()
        total = slots[0]
        for k in range(1, len(peers) + 1):
            total = total + slots[k]
        return total, result

    weight = jnp.zeros((32, 64), f32)
    mine, weight = exchange(mine, x_slots, x, x_peers, x_send, x_recv, lambda: count(0, weight))
    mine, weight = exchange(mine, z_slots, z, z_peers, z_send, z_recv, lambda: lax.fori_loop(1, 3, count, weight))
    both[core] = mine
    copy = pltpu.make_async_remote_copy(
        src_ref=both.at[core], dst_ref=both.at[core], send_sem=core_send.at[1], recv_sem=core_recv.at[1],
        device_id={"tm": other}, device_id_type=MESH,
    )
    copy.start()
    copy.wait()

    row = lax.broadcasted_iota(jnp.int32, (1, MODES, LANES), 1)
    for w in range(2):
        packed = both[w, MODES : MODES + 8, :]
        columns = []
        for k in range(MODES):
            top = jnp.broadcast_to(packed[:, k : k + 1], (8, LANES))
            low = jnp.broadcast_to(packed[:, MODES + k : MODES + k + 1], (8, LANES))
            columns.append(jnp.concatenate([top, low], axis=0))
        columns.append(both[w, 0:MODES, :])
        joined = jnp.stack(columns, axis=0)
        for c in range(MODES):
            factor = joined[0:1]
            pivot_row = joined[1:, c : c + 1, :] / factor[:, c : c + 1, :]
            joined = jnp.where(row == c, pivot_row, joined[1:] - factor * pivot_row)
        amps = joined[0]
        amps_ref[:, w * run : (w + 1) * run] = amps
        high, mid, low = split3(amps)
        left = jnp.concatenate([high, mid, low], axis=0)
        right = jnp.concatenate([shapes[w]] * 3, axis=0)
        fitted = lax.dot_general(left, right, (((0,), (0,)), ((), ())), preferred_element_type=f32)
        residual = data_ref[w * run : (w + 1) * run, :] - fitted
        tiles = residual.shape[1] // LANES
        for l in range(tiles):
            sent[pl.ds(w * run * tiles + l, run, stride=tiles), :] = residual[:, l * LANES : (l + 1) * LANES]

    piece = got.shape[1] // owners

    def move(d, carry):
        def one_peer(k, carry):
            peer = (tm + k) % owners
            pltpu.make_async_remote_copy(
                src_ref=sent.at[pl.ds((peer * dets + d) * piece, piece)], dst_ref=got.at[d, pl.ds(tm * piece, piece)],
                send_sem=move_send.at[d], recv_sem=move_recv.at[d], device_id={"tm": peer}, device_id_type=MESH,
            ).start()
            return carry

        lax.fori_loop(1, owners, one_peer, 0)
        got[d, pl.ds(pl.multiple_of(tm * piece, piece), piece), :] = sent[
            pl.ds(pl.multiple_of((tm * dets + d) * piece, piece), piece), :
        ]
        return carry

    lax.fori_loop(0, dets, move, 0)
    weight = count(dets - 1, weight)
    for fetch in fetches[2:]:
        fetch.wait()

    chunks = owners
    per = SIDE // chunks
    tiles = SIDE // LANES

    def weigh(d, total):
        arrived = pltpu.make_async_remote_copy(
            src_ref=got.at[d, pl.ds(0, (owners - 1) * piece)], dst_ref=got.at[d, pl.ds(0, (owners - 1) * piece)],
            send_sem=move_send.at[d], recv_sem=move_recv.at[d], device_id={"tm": other}, device_id_type=MESH,
        )
        arrived.wait()
        rows = []
        for j in range(per):
            rows.append(
                jnp.concatenate(
                    [got[d, pl.ds(j * tiles + h, chunks, stride=piece), :] for h in range(tiles)], axis=1
                )
            )
        signal = jnp.concatenate(rows, axis=0)
        spectrum = three((first_high[...], first_low[...]), split2(signal))
        real_y, imag_y, tail = spectrum[0:HALF], spectrum[HALF:], spectrum[HALF : HALF + 8]
        first_row = lax.broadcasted_iota(jnp.int32, (HALF, SIDE), 0) == 0
        imag_y = jnp.where(first_row, 0.0, imag_y)
        cos_main, sin_main = turn_cos[0:HALF, :], turn_sin[0:HALF, :]
        cos_tail, sin_tail = turn_cos[HALF:, :], turn_sin[HALF:, :]
        real_z = jnp.concatenate([real_y * cos_main + imag_y * sin_main, tail * cos_tail], axis=0)
        imag_z = jnp.concatenate([imag_y * cos_main - real_y * sin_main, -tail * sin_tail], axis=0)
        bins = three(
            split2(jnp.concatenate([real_z, imag_z], axis=1)), (second_high[...], second_low[...])
        )
        squared = squared_ref[...]
        knee = knee_ref[d]
        gain = squared / (white_ref[d] * (squared + knee * knee))
        bins = bins * jnp.concatenate([gain, gain], axis=1)
        back = three(split2(bins), (second_high[...], second_low[...]), NT)
        real_u, imag_u = back[:, 0:SIDE], back[:, SIDE:]
        real_w = real_u[0:HALF] * cos_main - imag_u[0:HALF] * sin_main
        imag_w = real_u[0:HALF] * sin_main + imag_u[0:HALF] * cos_main
        tail_w = (real_u[HALF:] * cos_tail - imag_u[HALF:] * sin_tail)[0:1]
        imag_w = jnp.where(first_row, jnp.broadcast_to(tail_w, (HALF, SIDE)), imag_w)
        joined = jnp.concatenate([real_w, imag_w], axis=0)
        output = three((last_high[...], last_low[...]), split2(joined))
        for h in range(tiles):
            part = output[:, h * LANES : (h + 1) * LANES]
            flat[pl.ds(h * dets + d, SIDE, stride=tiles * dets), :] = part
            rows_out[pl.ds(h, SIDE, stride=tiles), :] = part.astype(bf16).astype(f32)

        def value_of(turn):
            width = CHUNK // LANES
            values = rows_out[pl.ds(pl.multiple_of(turn * width, width), width), :].astype(bf16)
            return jnp.concatenate([values[l : l + 1, :] for l in range(width)], axis=1)

        return binned(d, total, value_of)

    sky = lax.fori_loop(0, dets, weigh, jnp.zeros((32, 64), f32))
    comb[0] = jnp.concatenate([sky[0:16], sky[16:32]], axis=1)
    comb[1] = jnp.concatenate([weight[0:16], weight[16:32]], axis=1)
    share = owners // 16
    ordered = maps_ref.shape[0]
    for r in range(ordered):
        tile = order_ref[r]
        maps_ref[r, 0:1, :] = comb[0, pl.ds(tile, 1), :]
        maps_ref[r, 1:2, :] = comb[1, pl.ds(tile, 1), :]

    def send(k, carry):
        peer = (tm + k) % owners
        pltpu.make_async_remote_copy(
            src_ref=maps_ref.at[peer // share], dst_ref=tm_slots.at[tm], send_sem=tm_send, recv_sem=tm_recv,
            device_id={"tm": peer}, device_id_type=MESH,
        ).start()
        return carry

    lax.fori_loop(1, owners, send, 0)
    tm_slots[tm] = maps_ref[tm // share]
    pltpu.make_async_remote_copy(
        src_ref=tm_slots.at[pl.ds(0, owners - 1)], dst_ref=tm_slots.at[pl.ds(0, owners - 1)],
        send_sem=tm_send, recv_sem=tm_recv, device_id={"tm": other}, device_id_type=MESH,
    ).wait()
    det_slots[det] = jnp.sum(tm_slots[...], axis=0)
    copies = []
    for k in range(1, det_size):
        copy = pltpu.make_async_remote_copy(
            src_ref=det_slots.at[det], dst_ref=det_slots.at[det], send_sem=det_send.at[k - 1],
            recv_sem=det_recv.at[k - 1], device_id={"det": (det + k) % det_size}, device_id_type=MESH,
        )
        copy.start()
        copies.append(copy)
    for copy in copies:
        copy.wait()
    total = det_slots[0]
    for k in range(1, det_size):
        total = total + det_slots[k]
    maps_ref[0] = total * scale


def whole(sizes, scale, owners, inputs):
    data, templates, wafer_of, knee_freq, white_level, tile_id, pixel_id, tile_order = inputs
    x_size, z_size, det_size = sizes
    rows, local = data.shape
    dets, samples = tile_id.shape
    stored = (tile_id, pixel_id) + tables(owners)
    vmem = pl.BlockSpec(memory_space=pltpu.VMEM)
    smem = pl.BlockSpec(memory_space=pltpu.SMEM)
    anywhere = pl.BlockSpec(memory_space=pl.ANY)
    part = (MODES + 8, LANES)
    dma = pltpu.SemaphoreType.DMA
    return pl.pallas_call(
        functools.partial(whole_kernel, sizes, scale),
        out_shape=(
            jax.ShapeDtypeStruct((MODES, rows), f32),
            jax.ShapeDtypeStruct((dets * samples // LANES, LANES), f32),
            jax.ShapeDtypeStruct((16, 2, LANES), f32),
        ),
        in_specs=[smem] * 4 + [vmem] * 2 + [anywhere] * len(stored),
        out_specs=[vmem] * 3,
        scratch_shapes=[pltpu.VMEM(a.shape, a.dtype) for a in stored]
        + [
            dma((len(stored),)),
            pltpu.VMEM((dets, samples), f32),
            pltpu.VMEM((dets, samples), f32),
            pltpu.VMEM((2,) + part, f32),
            pltpu.VMEM(part, f32),
            pltpu.VMEM((x_size,) + part, f32),
            pltpu.VMEM((z_size,) + part, f32),
            pltpu.VMEM((2,) + part, f32),
            pltpu.VMEM((rows * local // LANES, LANES), f32),
            pltpu.VMEM((dets, samples // LANES, LANES), f32),
            pltpu.VMEM((2, 16, LANES), f32),
            pltpu.VMEM((samples // LANES, LANES), f32),
            pltpu.VMEM((owners, 2, LANES), f32),
            pltpu.VMEM((det_size, 2, LANES), f32),
            dma((2,)),
            dma((2,)),
            dma((x_size - 1,)),
            dma((x_size - 1,)),
            dma((z_size - 1,)),
            dma((z_size - 1,)),
            dma((dets,)),
            dma((dets,)),
            dma,
            dma,
            dma((det_size - 1,)),
            dma((det_size - 1,)),
        ],
        compiler_params=pltpu.CompilerParams(collective_id=0, has_side_effects=True, vmem_limit_bytes=50 * 2**20),
        name="whole",
    )(wafer_of, knee_freq, white_level, tile_order, data, templates, *stored)


def shards(mesh, *inputs):
    owners = mesh.shape["tm"]
    det_size = mesh.shape["det"]
    dets, samples = inputs[5].shape
    cells = 16 * PIX
    scale = float(cells) / float(dets * owners * det_size * samples)
    fit_amps, flat, maps = whole((owners // 16, 8, det_size), scale, owners, inputs)
    weighted = flat.astype(bf16).reshape(samples // LANES, dets, LANES).transpose(1, 0, 2).reshape(dets, samples)
    share = cells // owners
    start = (lax.axis_index("tm") % (PIX // share)) * share
    own = lax.dynamic_slice(maps[0], (0, start), (2, share))
    return (fit_amps, weighted, own[0], own[1])


def solution(mesh):
    in_specs = (
        P("det", "tm"),
        P(None, None, "tm"),
        P("det"),
        P(("det", "tm")),
        P(("det", "tm")),
        P(("det", "tm"), None),
        P(("det", "tm"), None),
        P(),
    )
    out_specs = (P(None, "det"), P(("det", "tm"), None), P("tm"), P("tm"))
    return jax.shard_map(
        functools.partial(shards, mesh), mesh=mesh, in_specs=in_specs, out_specs=out_specs, check_vma=False
    )
```

```python
import functools
import math

import jax
import jax.numpy as jnp
import numpy as np
from jax import lax
from jax.experimental import pallas as pl
from jax.experimental.pallas import tpu as pltpu
from jax.sharding import PartitionSpec as P

PIX = 128
MODES = 16
LANES = 128
SIDE = 256
HALF = SIDE // 2
ROWS = HALF + 8
sample_rate = 200.0
f32 = jnp.float32
bf16 = jnp.bfloat16
MESH = pl.DeviceIdType.MESH
NT = (((1,), (1,)), ((), ()))
NN = (((1,), (0,)), ((), ()))


def mm(a, b, dims=NN):
    return lax.dot_general(a, b, dims, preferred_element_type=f32)


def split2(x):
    high = x.astype(bf16)
    low = (x - high.astype(f32)).astype(bf16)
    return high, low


def split3(x):
    high = x.astype(bf16)
    rest = x - high.astype(f32)
    mid = rest.astype(bf16)
    low = (rest - mid.astype(f32)).astype(bf16)
    return high, mid, low


def tables(chunks):
    full = SIDE * SIDE
    per = SIDE // chunks
    ramp = np.arange(SIDE)
    order = np.array([per * s + j for j in range(per) for s in range(chunks)])
    angle = 2.0 * np.pi / SIDE * (np.outer(ramp, ramp) % SIDE)
    cos, sin = np.cos(angle), np.sin(angle)
    first = np.concatenate([cos[:HALF], -sin[:HALF]], axis=0)
    first[HALF] = cos[HALF]
    second = np.block([[cos, -sin], [sin, cos]])
    weight = np.full((HALF,), 2.0)
    weight[0] = 1.0
    last = np.concatenate([cos[:, :HALF] * weight, -sin[:, :HALF] * weight], axis=1)
    last[:, HALF] = cos[:, HALF]
    k = np.arange(ROWS)
    turn = 2.0 * np.pi / full * np.outer(k, ramp)
    valid = (k <= HALF)[:, None]
    turn_cos, turn_sin = np.cos(turn) * valid, np.sin(turn) * valid
    bins = k[:, None] + SIDE * ramp[None, :]
    folded = np.minimum(bins, full - bins).astype(np.float32)
    frequency = folded * np.float32(sample_rate / full)
    squared = np.where(valid, frequency * frequency, np.float32(0)).astype(np.float32)

    def halves(a):
        a = a.astype(np.float32)
        high = a.astype(jnp.bfloat16)
        return high, (a - high.astype(np.float32)).astype(jnp.bfloat16)

    return (
        *halves(first[:, order]),
        *halves(second),
        *halves(last / full),
        turn_cos.astype(np.float32),
        turn_sin.astype(np.float32),
        squared,
    )


def three(left, right, dims=NN):
    return mm(left[0], right[0], dims) + mm(left[0], right[1], dims) + mm(left[1], right[0], dims)


CHUNK = 8192
f8 = jnp.float8_e4m3fn


def whole_kernel(
    sizes, scale, wafer_ref, knee_ref, white_ref, order_ref, data_ref, templates_ref, *refs
):
    x_size, z_size, det_size = sizes
    stored, refs = refs[:11], refs[11:]
    amps_ref, flat_ref, maps_ref = refs[:3]
    held, refs = refs[3:14], refs[14:]
    (
        fetch_sem, left_ids, right_ids, parts, near_slots, z_slots, both, sent, got, flat, comb, rows_out,
        tm_slots, det_slots, near_send, near_recv, z_send, z_recv, back_send, back_recv, move_send, move_recv,
        tm_send, tm_recv, det_send, det_recv, flat_sem,
    ) = refs
    tile_ref, pixel_ref = held[:2]
    first_high, first_low, second_high, second_low, last_high, last_low, turn_cos, turn_sin, squared_ref = held[2:]
    dets, samples = tile_ref.shape
    owners = x_size * z_size * 2
    tm = lax.axis_index("tm")
    det = lax.axis_index("det")
    core = tm % 2
    z = (tm // 2) % z_size
    x = tm // (2 * z_size)

    def index_of(x_at, z_at, core_at):
        return (x_at * z_size + z_at) * 2 + core_at

    near_size = 2 * x_size
    near = x * 2 + core
    near_at = [(near + k) % near_size for k in range(1, near_size)]
    near_peers = [index_of(at // 2, z, at % 2) for at in near_at]
    z_peers = [index_of(x, (z + k) % z_size, core) for k in range(1, z_size)]
    peers = near_peers + z_peers
    other = near_peers[0]
    barrier = pltpu.get_barrier_semaphore()
    for peer in peers:
        pl.semaphore_signal(barrier, inc=1, device_id={"tm": peer}, device_id_type=MESH)
    for k in range(1, det_size):
        pl.semaphore_signal(barrier, inc=1, device_id={"det": (det + k) % det_size}, device_id_type=MESH)
    fetches = [
        pltpu.make_async_copy(stored[k], held[k], fetch_sem.at[k]) for k in range(len(stored))
    ]
    for fetch in fetches:
        fetch.start()

    run = data_ref.shape[0] // 2
    shapes = []
    for w in range(2):
        shape = templates_ref[wafer_ref[w * run]]
        shapes.append(shape)
        high, mid, low = split3(data_ref[w * run : (w + 1) * run, :])
        projected = mm(shape, high, NT) + mm(shape, mid, NT) + mm(shape, low, NT)
        gram = mm(shape, shape, NT)
        pad = jnp.zeros((8, LANES - 2 * MODES), f32)
        parts[w * 4] = projected[0:8]
        parts[w * 4 + 1] = projected[8:16]
        parts[w * 4 + 2] = jnp.concatenate([gram[0:8], gram[8:16], pad], axis=1)
        parts[w * 4 + 3] = jnp.zeros((8, LANES), f32)

    pl.semaphore_wait(barrier, len(peers) + det_size - 1)
    near_copies = []
    for k in range(near_size - 1):
        copy = pltpu.make_async_remote_copy(
            src_ref=parts.at[near_at[k]], dst_ref=near_slots.at[near], send_sem=near_send.at[k],
            recv_sem=near_recv.at[k], device_id={"tm": near_peers[k]}, device_id_type=MESH,
        )
        copy.start()
        near_copies.append(copy)
    near_slots[near] = parts[near]

    def ids(turn, carry):
        span = pl.ds(pl.multiple_of(turn * CHUNK, CHUNK), CHUNK)
        tiles = tile_ref[:, span]
        pixels = pixel_ref[:, span]
        left_ids[:, span] = (tiles + 16 * (pixels >> 6)).astype(f32)
        right_ids[:, span] = (pixels & 63).astype(f32)
        return carry

    for fetch in fetches[:2]:
        fetch.wait()
    lax.fori_loop(0, samples // CHUNK, ids, 0)
    one, zero = jnp.ones((), bf16), jnp.zeros((), bf16)

    def ramp(rows):
        return lax.broadcasted_iota(jnp.int32, (rows, CHUNK), 0).astype(f32).astype(bf16)

    def binned(d, total, value_of):
        def step(turn, total):
            span = pl.ds(pl.multiple_of(turn * CHUNK, CHUNK), CHUNK)
            left_id = left_ids[pl.ds(d, 1), span].astype(bf16)
            right_id = right_ids[pl.ds(d, 1), span].astype(bf16)
            left = jnp.where(left_id == ramp(32), value_of(turn), zero)
            right = jnp.where(right_id == ramp(64), one, zero).astype(f8)
            return total + mm(left, right, NT)

        return lax.fori_loop(0, samples // CHUNK, step, total)

    def count(d, total):
        inverse = (jnp.ones((1, 64), f32) / jnp.full((1, 64), white_ref[d], f32)).astype(bf16).astype(f32)
        return total + binned(d, jnp.zeros((32, 64), f32), lambda turn: one) * inverse

    def spread(slots, place, peers, send_sem, recv_sem):
        copies = []
        for k, peer in enumerate(peers):
            copy = pltpu.make_async_remote_copy(
                src_ref=slots.at[place], dst_ref=slots.at[place], send_sem=send_sem.at[k], recv_sem=recv_sem.at[k],
                device_id={"tm": peer}, device_id_type=MESH,
            )
            copy.start()
            copies.append(copy)
        return copies

    def gathered(slots, copies):
        for copy in copies:
            copy.wait()
        total = slots[0]
        for k in range(1, len(copies) + 1):
            total = total + slots[k]
        return total

    weight = count(0, jnp.zeros((32, 64), f32))
    z_slots[z] = gathered(near_slots, near_copies)
    copies = spread(z_slots, z, z_peers, z_send, z_recv)
    weight = count(1, weight)
    both[near] = gathered(z_slots, copies)
    copies = spread(both, near, near_peers, back_send, back_recv)
    for copy in copies:
        copy.wait()

    row = lax.broadcasted_iota(jnp.int32, (1, MODES, LANES), 1)
    for w in range(2):
        packed = both[w * 4 + 2]
        columns = []
        for k in range(MODES):
            top = jnp.broadcast_to(packed[:, k : k + 1], (8, LANES))
            low = jnp.broadcast_to(packed[:, MODES + k : MODES + k + 1], (8, LANES))
            columns.append(jnp.concatenate([top, low], axis=0))
        columns.append(jnp.concatenate([both[w * 4], both[w * 4 + 1]], axis=0))
        joined = jnp.stack(columns, axis=0)
        for c in range(MODES):
            factor = joined[0:1]
            pivot_row = joined[1:, c : c + 1, :] / factor[:, c : c + 1, :]
            joined = jnp.where(row == c, pivot_row, joined[1:] - factor * pivot_row)
        amps = joined[0]
        amps_ref[:, w * run : (w + 1) * run] = amps
        high, mid, low = split3(amps)
        left = jnp.concatenate([high, mid, low], axis=0)
        right = jnp.concatenate([shapes[w]] * 3, axis=0)
        fitted = lax.dot_general(left, right, (((0,), (0,)), ((), ())), preferred_element_type=f32)
        residual = data_ref[w * run : (w + 1) * run, :] - fitted
        tiles = residual.shape[1] // LANES
        for l in range(tiles):
            sent[pl.ds(w * run * tiles + l, run, stride=tiles), :] = residual[:, l * LANES : (l + 1) * LANES]

    piece = got.shape[1] // owners

    def move(d, carry):
        def one_peer(k, carry):
            peer = (tm + k) % owners
            pltpu.make_async_remote_copy(
                src_ref=sent.at[pl.ds((peer * dets + d) * piece, piece)], dst_ref=got.at[d, pl.ds(tm * piece, piece)],
                send_sem=move_send.at[d], recv_sem=move_recv.at[d], device_id={"tm": peer}, device_id_type=MESH,
            ).start()
            return carry

        lax.fori_loop(1, owners, one_peer, 0)
        got[d, pl.ds(pl.multiple_of(tm * piece, piece), piece), :] = sent[
            pl.ds(pl.multiple_of((tm * dets + d) * piece, piece), piece), :
        ]
        return carry

    lax.fori_loop(0, dets, move, 0)
    weight = lax.fori_loop(2, dets, count, weight)
    for fetch in fetches[2:]:
        fetch.wait()

    chunks = owners
    per = SIDE // chunks
    tiles = SIDE // LANES

    def weigh(d, total):
        arrived = pltpu.make_async_remote_copy(
            src_ref=got.at[d, pl.ds(0, (owners - 1) * piece)], dst_ref=got.at[d, pl.ds(0, (owners - 1) * piece)],
            send_sem=move_send.at[d], recv_sem=move_recv.at[d], device_id={"tm": other}, device_id_type=MESH,
        )
        arrived.wait()
        rows = []
        for j in range(per):
            rows.append(
                jnp.concatenate(
                    [got[d, pl.ds(j * tiles + h, chunks, stride=piece), :] for h in range(tiles)], axis=1
                )
            )
        signal = jnp.concatenate(rows, axis=0)
        spectrum = three((first_high[...], first_low[...]), split2(signal))
        real_y, imag_y, tail = spectrum[0:HALF], spectrum[HALF:], spectrum[HALF : HALF + 8]
        first_row = lax.broadcasted_iota(jnp.int32, (HALF, SIDE), 0) == 0
        imag_y = jnp.where(first_row, 0.0, imag_y)
        cos_main, sin_main = turn_cos[0:HALF, :], turn_sin[0:HALF, :]
        cos_tail, sin_tail = turn_cos[HALF:, :], turn_sin[HALF:, :]
        real_z = jnp.concatenate([real_y * cos_main + imag_y * sin_main, tail * cos_tail], axis=0)
        imag_z = jnp.concatenate([imag_y * cos_main - real_y * sin_main, -tail * sin_tail], axis=0)
        bins = three(
            split2(jnp.concatenate([real_z, imag_z], axis=1)), (second_high[...], second_low[...])
        )
        squared = squared_ref[...]
        knee = knee_ref[d]
        gain = squared / (white_ref[d] * (squared + knee * knee))
        bins = bins * jnp.concatenate([gain, gain], axis=1)
        back = three(split2(bins), (second_high[...], second_low[...]), NT)
        real_u, imag_u = back[:, 0:SIDE], back[:, SIDE:]
        real_w = real_u[0:HALF] * cos_main - imag_u[0:HALF] * sin_main
        imag_w = real_u[0:HALF] * sin_main + imag_u[0:HALF] * cos_main
        tail_w = (real_u[HALF:] * cos_tail - imag_u[HALF:] * sin_tail)[0:1]
        imag_w = jnp.where(first_row, jnp.broadcast_to(tail_w, (HALF, SIDE)), imag_w)
        joined = jnp.concatenate([real_w, imag_w], axis=0)
        output = three((last_high[...], last_low[...]), split2(joined))
        for h in range(tiles):
            part = output[:, h * LANES : (h + 1) * LANES]
            flat[pl.ds(h * dets + d, SIDE, stride=tiles * dets), :] = part
            rows_out[pl.ds(h, SIDE, stride=tiles), :] = part.astype(bf16).astype(f32)

        def value_of(turn):
            width = CHUNK // LANES
            values = rows_out[pl.ds(pl.multiple_of(turn * width, width), width), :].astype(bf16)
            return jnp.concatenate([values[l : l + 1, :] for l in range(width)], axis=1)

        return binned(d, total, value_of)

    sky = lax.fori_loop(0, dets, weigh, jnp.zeros((32, 64), f32))
    flat_out = pltpu.make_async_copy(flat, flat_ref, flat_sem)
    flat_out.start()
    comb[0] = jnp.concatenate([sky[0:16], sky[16:32]], axis=1)
    comb[1] = jnp.concatenate([weight[0:16], weight[16:32]], axis=1)
    share = owners // 16
    ordered = maps_ref.shape[0]
    for r in range(ordered):
        tile = order_ref[r]
        maps_ref[r, 0:1, :] = comb[0, pl.ds(tile, 1), :]
        maps_ref[r, 1:2, :] = comb[1, pl.ds(tile, 1), :]

    def send(k, carry):
        peer = (tm + k) % owners
        pltpu.make_async_remote_copy(
            src_ref=maps_ref.at[peer // share], dst_ref=tm_slots.at[tm], send_sem=tm_send, recv_sem=tm_recv,
            device_id={"tm": peer}, device_id_type=MESH,
        ).start()
        return carry

    lax.fori_loop(1, owners, send, 0)
    tm_slots[tm] = maps_ref[tm // share]
    pltpu.make_async_remote_copy(
        src_ref=tm_slots.at[pl.ds(0, owners - 1)], dst_ref=tm_slots.at[pl.ds(0, owners - 1)],
        send_sem=tm_send, recv_sem=tm_recv, device_id={"tm": other}, device_id_type=MESH,
    ).wait()
    det_slots[det] = jnp.sum(tm_slots[...], axis=0)
    copies = []
    for k in range(1, det_size):
        copy = pltpu.make_async_remote_copy(
            src_ref=det_slots.at[det], dst_ref=det_slots.at[det], send_sem=det_send.at[k - 1],
            recv_sem=det_recv.at[k - 1], device_id={"det": (det + k) % det_size}, device_id_type=MESH,
        )
        copy.start()
        copies.append(copy)
    for copy in copies:
        copy.wait()
    total = det_slots[0]
    for k in range(1, det_size):
        total = total + det_slots[k]
    maps_ref[0] = total * scale
    flat_out.wait()


def whole(sizes, scale, owners, inputs):
    data, templates, wafer_of, knee_freq, white_level, tile_id, pixel_id, tile_order = inputs
    x_size, z_size, det_size = sizes
    rows, local = data.shape
    dets, samples = tile_id.shape
    stored = (tile_id, pixel_id) + tables(owners)
    vmem = pl.BlockSpec(memory_space=pltpu.VMEM)
    smem = pl.BlockSpec(memory_space=pltpu.SMEM)
    anywhere = pl.BlockSpec(memory_space=pltpu.HBM)
    part = (8, LANES)
    near_size = 2 * x_size
    dma = pltpu.SemaphoreType.DMA
    return pl.pallas_call(
        functools.partial(whole_kernel, sizes, scale),
        out_shape=(
            jax.ShapeDtypeStruct((MODES, rows), f32),
            jax.ShapeDtypeStruct((dets * samples // LANES, LANES), f32),
            jax.ShapeDtypeStruct((16, 2, LANES), f32),
        ),
        in_specs=[smem] * 4 + [vmem] * 2 + [anywhere] * len(stored),
        out_specs=[vmem, anywhere, vmem],
        scratch_shapes=[pltpu.VMEM(a.shape, a.dtype) for a in stored]
        + [
            dma((len(stored),)),
            pltpu.VMEM((dets, samples), f32),
            pltpu.VMEM((dets, samples), f32),
            pltpu.VMEM((near_size,) + part, f32),
            pltpu.VMEM((near_size,) + part, f32),
            pltpu.VMEM((z_size,) + part, f32),
            pltpu.VMEM((near_size,) + part, f32),
            pltpu.VMEM((rows * local // LANES, LANES), f32),
            pltpu.VMEM((dets, samples // LANES, LANES), f32),
            pltpu.VMEM((dets * samples // LANES, LANES), f32),
            pltpu.VMEM((2, 16, LANES), f32),
            pltpu.VMEM((samples // LANES, LANES), f32),
            pltpu.VMEM((owners, 2, LANES), f32),
            pltpu.VMEM((det_size, 2, LANES), f32),
            dma((near_size - 1,)),
            dma((near_size - 1,)),
            dma((z_size - 1,)),
            dma((z_size - 1,)),
            dma((near_size - 1,)),
            dma((near_size - 1,)),
            dma((dets,)),
            dma((dets,)),
            dma,
            dma,
            dma((det_size - 1,)),
            dma((det_size - 1,)),
            dma,
        ],
        compiler_params=pltpu.CompilerParams(collective_id=0, has_side_effects=True, vmem_limit_bytes=67043328),
        name="whole",
    )(wafer_of, knee_freq, white_level, tile_order, data, templates, *stored)


def shards(mesh, *inputs):
    owners = mesh.shape["tm"]
    det_size = mesh.shape["det"]
    dets, samples = inputs[5].shape
    cells = 16 * PIX
    scale = float(cells) / float(dets * owners * det_size * samples)
    fit_amps, flat, maps = whole((owners // 16, 8, det_size), scale, owners, inputs)
    weighted = flat.astype(bf16).reshape(samples // LANES, dets, LANES).transpose(1, 0, 2).reshape(dets, samples)
    share = cells // owners
    start = (lax.axis_index("tm") % (PIX // share)) * share
    own = lax.dynamic_slice(maps[0], (0, start), (2, share))
    return (fit_amps, weighted, own[0], own[1])


def solution(mesh):
    in_specs = (
        P("det", "tm"),
        P(None, None, "tm"),
        P("det"),
        P(("det", "tm")),
        P(("det", "tm")),
        P(("det", "tm"), None),
        P(("det", "tm"), None),
        P(),
    )
    out_specs = (P(None, "det"), P(("det", "tm"), None), P("tm"), P("tm"))
    return jax.shard_map(
        functools.partial(shards, mesh), mesh=mesh, in_specs=in_specs, out_specs=out_specs, check_vma=False
    )
```

```python
import functools
import math

import jax
import jax.numpy as jnp
import numpy as np
from jax import lax
from jax.experimental import pallas as pl
from jax.experimental.pallas import tpu as pltpu
from jax.sharding import PartitionSpec as P

PIX = 128
MODES = 16
LANES = 128
SIDE = 256
HALF = SIDE // 2
ROWS = HALF + 8
sample_rate = 200.0
f32 = jnp.float32
bf16 = jnp.bfloat16
MESH = pl.DeviceIdType.MESH
NT = (((1,), (1,)), ((), ()))
NN = (((1,), (0,)), ((), ()))


def mm(a, b, dims=NN):
    return lax.dot_general(a, b, dims, preferred_element_type=f32)


def split2(x):
    high = x.astype(bf16)
    low = (x - high.astype(f32)).astype(bf16)
    return high, low


def split3(x):
    high = x.astype(bf16)
    rest = x - high.astype(f32)
    mid = rest.astype(bf16)
    low = (rest - mid.astype(f32)).astype(bf16)
    return high, mid, low


def tables(chunks):
    full = SIDE * SIDE
    per = SIDE // chunks
    ramp = np.arange(SIDE)
    order = np.array([per * s + j for j in range(per) for s in range(chunks)])
    angle = 2.0 * np.pi / SIDE * (np.outer(ramp, ramp) % SIDE)
    cos, sin = np.cos(angle), np.sin(angle)
    first = np.concatenate([cos[:HALF], -sin[:HALF]], axis=0)
    first[HALF] = cos[HALF]
    second = np.block([[cos, -sin], [sin, cos]])
    weight = np.full((HALF,), 2.0)
    weight[0] = 1.0
    last = np.concatenate([cos[:, :HALF] * weight, -sin[:, :HALF] * weight], axis=1)
    last[:, HALF] = cos[:, HALF]
    k = np.arange(ROWS)
    turn = 2.0 * np.pi / full * np.outer(k, ramp)
    valid = (k <= HALF)[:, None]
    turn_cos, turn_sin = np.cos(turn) * valid, np.sin(turn) * valid
    bins = k[:, None] + SIDE * ramp[None, :]
    folded = np.minimum(bins, full - bins).astype(np.float32)
    frequency = folded * np.float32(sample_rate / full)
    squared = np.where(valid, frequency * frequency, np.float32(0)).astype(np.float32)

    def halves(a):
        a = a.astype(np.float32)
        high = a.astype(jnp.bfloat16)
        return high, (a - high.astype(np.float32)).astype(jnp.bfloat16)

    return (
        *halves(first[:, order]),
        *halves(second),
        *halves(last / full),
        turn_cos.astype(np.float32),
        turn_sin.astype(np.float32),
        squared,
    )


def three(left, right, dims=NN):
    return mm(left[0], right[0], dims) + mm(left[0], right[1], dims) + mm(left[1], right[0], dims)


CHUNK = 8192
f8 = jnp.float8_e4m3fn


def whole_kernel(
    sizes, scale, wafer_ref, knee_ref, white_ref, order_ref, data_ref, templates_ref, *refs
):
    x_size, z_size, det_size = sizes
    stored, refs = refs[:11], refs[11:]
    amps_ref, flat_ref, own_ref = refs[:3]
    held, refs = refs[3:14], refs[14:]
    (
        fetch_sem, left_ids, right_ids, hots, parts, near_slots, z_slots, both, sent, got, flat, rounded, comb, maps_ref, rows_out,
        tm_slots, det_slots, near_send, near_recv, z_send, z_recv, back_send, back_recv, move_send, move_recv,
        tm_send, tm_recv, det_send, det_recv, flat_sem,
    ) = refs
    tile_ref, pixel_ref = held[:2]
    first_high, first_low, second_high, second_low, last_high, last_low, turn_cos, turn_sin, squared_ref = held[2:]
    dets, samples = tile_ref.shape
    owners = x_size * z_size * 2
    tm = lax.axis_index("tm")
    det = lax.axis_index("det")
    core = tm % 2
    z = (tm // 2) % z_size
    x = tm // (2 * z_size)

    def index_of(x_at, z_at, core_at):
        return (x_at * z_size + z_at) * 2 + core_at

    near_size = 2 * x_size
    near = x * 2 + core
    near_at = [(near + k) % near_size for k in range(1, near_size)]
    near_peers = [index_of(at // 2, z, at % 2) for at in near_at]
    z_peers = [index_of(x, (z + k) % z_size, core) for k in range(1, z_size)]
    peers = near_peers + z_peers
    other = near_peers[0]
    barrier = pltpu.get_barrier_semaphore()
    for peer in peers:
        pl.semaphore_signal(barrier, inc=1, device_id={"tm": peer}, device_id_type=MESH)
    for k in range(1, det_size):
        pl.semaphore_signal(barrier, inc=1, device_id={"det": (det + k) % det_size}, device_id_type=MESH)
    fetches = [
        pltpu.make_async_copy(stored[k], held[k], fetch_sem.at[k]) for k in range(len(stored))
    ]
    for fetch in fetches:
        fetch.start()

    run = data_ref.shape[0] // 2
    shapes = []
    for w in range(2):
        shape = templates_ref[wafer_ref[w * run]]
        shapes.append(shape)
        high, mid, low = split3(data_ref[w * run : (w + 1) * run, :])
        projected = mm(shape, high, NT) + mm(shape, mid, NT) + mm(shape, low, NT)
        gram = mm(shape, shape, NT)
        pad = jnp.zeros((8, LANES - 2 * MODES), f32)
        parts[w * 4] = projected[0:8]
        parts[w * 4 + 1] = projected[8:16]
        parts[w * 4 + 2] = jnp.concatenate([gram[0:8], gram[8:16], pad], axis=1)
        parts[w * 4 + 3] = jnp.zeros((8, LANES), f32)

    pl.semaphore_wait(barrier, len(peers) + det_size - 1)
    near_copies = []
    for k in range(near_size - 1):
        copy = pltpu.make_async_remote_copy(
            src_ref=parts.at[near_at[k]], dst_ref=near_slots.at[near], send_sem=near_send.at[k],
            recv_sem=near_recv.at[k], device_id={"tm": near_peers[k]}, device_id_type=MESH,
        )
        copy.start()
        near_copies.append(copy)
    near_slots[near] = parts[near]

    def ids(turn, carry):
        span = pl.ds(pl.multiple_of(turn * CHUNK, CHUNK), CHUNK)
        tiles = tile_ref[:, span]
        pixels = pixel_ref[:, span]
        left_ids[:, span] = (tiles + 16 * (pixels >> 6)).astype(f32)
        right_ids[:, span] = (pixels & 63).astype(f32)
        return carry

    for fetch in fetches[:2]:
        fetch.wait()
    lax.fori_loop(0, samples // CHUNK, ids, 0)
    one, zero = jnp.ones((), bf16), jnp.zeros((), bf16)

    def ramp(rows):
        return lax.broadcasted_iota(jnp.int32, (rows, CHUNK), 0).astype(f32).astype(bf16)

    def left_hot(d, span, value):
        left_id = left_ids[pl.ds(d, 1), span].astype(bf16)
        return jnp.where(left_id == ramp(32), value, zero)

    def count(d, total):
        def step(turn, total):
            span = pl.ds(pl.multiple_of(turn * CHUNK, CHUNK), CHUNK)
            right_id = right_ids[pl.ds(d, 1), span].astype(bf16)
            right = jnp.where(right_id == ramp(64), one, zero).astype(f8)
            hots[d, :, span] = right
            return total + mm(left_hot(d, span, one), right, NT)

        inverse = (jnp.ones((1, 64), f32) / jnp.full((1, 64), white_ref[d], f32)).astype(bf16).astype(f32)
        return total + lax.fori_loop(0, samples // CHUNK, step, jnp.zeros((32, 64), f32)) * inverse

    def spread(slots, place, peers, send_sem, recv_sem):
        copies = []
        for k, peer in enumerate(peers):
            copy = pltpu.make_async_remote_copy(
                src_ref=slots.at[place], dst_ref=slots.at[place], send_sem=send_sem.at[k], recv_sem=recv_sem.at[k],
                device_id={"tm": peer}, device_id_type=MESH,
            )
            copy.start()
            copies.append(copy)
        return copies

    def gathered(slots, copies):
        for copy in copies:
            copy.wait()
        total = slots[0]
        for k in range(1, len(copies) + 1):
            total = total + slots[k]
        return total

    weight = count(0, jnp.zeros((32, 64), f32))
    z_slots[z] = gathered(near_slots, near_copies)
    copies = spread(z_slots, z, z_peers, z_send, z_recv)
    weight = count(1, weight)
    both[near] = gathered(z_slots, copies)
    copies = spread(both, near, near_peers, back_send, back_recv)
    for copy in copies:
        copy.wait()

    row = lax.broadcasted_iota(jnp.int32, (1, MODES, LANES), 1)
    for w in range(2):
        packed = both[w * 4 + 2]
        columns = []
        for k in range(MODES):
            top = jnp.broadcast_to(packed[:, k : k + 1], (8, LANES))
            low = jnp.broadcast_to(packed[:, MODES + k : MODES + k + 1], (8, LANES))
            columns.append(jnp.concatenate([top, low], axis=0))
        columns.append(jnp.concatenate([both[w * 4], both[w * 4 + 1]], axis=0))
        joined = jnp.stack(columns, axis=0)
        for c in range(MODES):
            factor = joined[0:1]
            pivot_row = joined[1:, c : c + 1, :] / factor[:, c : c + 1, :]
            joined = jnp.where(row == c, pivot_row, joined[1:] - factor * pivot_row)
        amps = joined[0]
        amps_ref[:, w * run : (w + 1) * run] = amps
        high, mid, low = split3(amps)
        left = jnp.concatenate([high, mid, low], axis=0)
        right = jnp.concatenate([shapes[w]] * 3, axis=0)
        fitted = lax.dot_general(left, right, (((0,), (0,)), ((), ())), preferred_element_type=f32)
        residual = data_ref[w * run : (w + 1) * run, :] - fitted
        tiles = residual.shape[1] // LANES
        for l in range(tiles):
            sent[pl.ds(w * run * tiles + l, run, stride=tiles), :] = residual[:, l * LANES : (l + 1) * LANES]

    piece = got.shape[1] // owners

    def move(d, carry):
        def one_peer(k, carry):
            peer = (tm + k) % owners
            pltpu.make_async_remote_copy(
                src_ref=sent.at[pl.ds((peer * dets + d) * piece, piece)], dst_ref=got.at[d, pl.ds(tm * piece, piece)],
                send_sem=move_send.at[d], recv_sem=move_recv.at[d], device_id={"tm": peer}, device_id_type=MESH,
            ).start()
            return carry

        lax.fori_loop(1, owners, one_peer, 0)
        got[d, pl.ds(pl.multiple_of(tm * piece, piece), piece), :] = sent[
            pl.ds(pl.multiple_of((tm * dets + d) * piece, piece), piece), :
        ]
        return carry

    lax.fori_loop(0, dets, move, 0)
    weight = lax.fori_loop(2, dets, count, weight)
    for fetch in fetches[2:]:
        fetch.wait()

    chunks = owners
    per = SIDE // chunks
    tiles = SIDE // LANES

    def turned(ref):
        upper = jnp.concatenate([ref[0:SIDE, 0:SIDE], ref[SIDE:, 0:SIDE]], axis=1)
        lower = jnp.concatenate([ref[0:SIDE, SIDE:], ref[SIDE:, SIDE:]], axis=1)
        return jnp.concatenate([upper, lower], axis=0)

    def weigh(d, total):
        arrived = pltpu.make_async_remote_copy(
            src_ref=got.at[d, pl.ds(0, (owners - 1) * piece)], dst_ref=got.at[d, pl.ds(0, (owners - 1) * piece)],
            send_sem=move_send.at[d], recv_sem=move_recv.at[d], device_id={"tm": other}, device_id_type=MESH,
        )
        arrived.wait()
        rows = []
        for j in range(per):
            rows.append(
                jnp.concatenate(
                    [got[d, pl.ds(j * tiles + h, chunks, stride=piece), :] for h in range(tiles)], axis=1
                )
            )
        signal = jnp.concatenate(rows, axis=0)
        spectrum = three((first_high[...], first_low[...]), split2(signal))
        real_y, imag_y, tail = spectrum[0:HALF], spectrum[HALF:], spectrum[HALF : HALF + 8]
        first_row = lax.broadcasted_iota(jnp.int32, (HALF, SIDE), 0) == 0
        imag_y = jnp.where(first_row, 0.0, imag_y)
        cos_main, sin_main = turn_cos[0:HALF, :], turn_sin[0:HALF, :]
        cos_tail, sin_tail = turn_cos[HALF:, :], turn_sin[HALF:, :]
        real_z = jnp.concatenate([real_y * cos_main + imag_y * sin_main, tail * cos_tail], axis=0)
        imag_z = jnp.concatenate([imag_y * cos_main - real_y * sin_main, -tail * sin_tail], axis=0)
        bins = three(
            split2(jnp.concatenate([real_z, imag_z], axis=1)), (second_high[...], second_low[...])
        )
        squared = squared_ref[...]
        knee = knee_ref[d]
        gain = squared / (white_ref[d] * (squared + knee * knee))
        bins = bins * jnp.concatenate([gain, gain], axis=1)
        back = three(split2(bins), (turned(second_high), turned(second_low)))
        real_u, imag_u = back[:, 0:SIDE], back[:, SIDE:]
        real_w = real_u[0:HALF] * cos_main - imag_u[0:HALF] * sin_main
        imag_w = real_u[0:HALF] * sin_main + imag_u[0:HALF] * cos_main
        tail_w = (real_u[HALF:] * cos_tail - imag_u[HALF:] * sin_tail)[0:1]
        imag_w = jnp.where(first_row, jnp.broadcast_to(tail_w, (HALF, SIDE)), imag_w)
        joined = jnp.concatenate([real_w, imag_w], axis=0)
        output = three((last_high[...], last_low[...]), split2(joined))
        for h in range(tiles):
            part = output[:, h * LANES : (h + 1) * LANES]
            flat[pl.ds(h * dets + d, SIDE, stride=tiles * dets), :] = part
            rows_out[pl.ds(h, SIDE, stride=tiles), :] = part.astype(bf16).astype(f32)

        def step(turn, total):
            span = pl.ds(pl.multiple_of(turn * CHUNK, CHUNK), CHUNK)
            width = CHUNK // LANES
            values = rows_out[pl.ds(pl.multiple_of(turn * width, width), width), :].astype(bf16)
            value = jnp.concatenate([values[l : l + 1, :] for l in range(width)], axis=1)
            return total + mm(left_hot(d, span, value), hots[d, :, span], NT)

        return lax.fori_loop(0, samples // CHUNK, step, total)

    sky = lax.fori_loop(0, dets, weigh, jnp.zeros((32, 64), f32))
    rounded[...] = flat[...].astype(bf16)
    flat_out = pltpu.make_async_copy(rounded, flat_ref, flat_sem)
    flat_out.start()
    comb[0] = jnp.concatenate([sky[0:16], sky[16:32]], axis=1)
    comb[1] = jnp.concatenate([weight[0:16], weight[16:32]], axis=1)
    share = owners // 16
    ordered = maps_ref.shape[0]
    for r in range(ordered):
        tile = order_ref[r]
        maps_ref[r, 0:1, :] = comb[0, pl.ds(tile, 1), :]
        maps_ref[r, 1:2, :] = comb[1, pl.ds(tile, 1), :]

    def send(dx, dz, dc):
        peer = index_of((x + dx) % x_size, (z + dz) % z_size, (core + dc) % 2)
        pltpu.make_async_remote_copy(
            src_ref=maps_ref.at[peer // share], dst_ref=tm_slots.at[tm], send_sem=tm_send, recv_sem=tm_recv,
            device_id={"tm": peer}, device_id_type=MESH,
        ).start()

    def far_first(size):
        return sorted(range(size), key=lambda k: -min(k, size - k))

    near_steps = [(dx, dc) for dx in far_first(x_size) for dc in (1, 0)]

    def send_far(j, carry):
        dz = z_size // 2 + (j + 1) // 2 * (2 * ((j + 1) % 2) - 1)
        for dx, dc in near_steps:
            send(dx, dz, dc)
        return carry

    lax.fori_loop(0, z_size - 1, send_far, 0)
    for dx, dc in near_steps:
        if (dx, dc) != (0, 0):
            send(dx, 0, dc)
    tm_slots[tm] = maps_ref[tm // share]
    pltpu.make_async_remote_copy(
        src_ref=tm_slots.at[pl.ds(0, owners - 1)], dst_ref=tm_slots.at[pl.ds(0, owners - 1)],
        send_sem=tm_send, recv_sem=tm_recv, device_id={"tm": other}, device_id_type=MESH,
    ).wait()
    det_slots[det] = jnp.sum(tm_slots[...], axis=0)
    copies = []
    for k in range(1, det_size):
        copy = pltpu.make_async_remote_copy(
            src_ref=det_slots.at[det], dst_ref=det_slots.at[det], send_sem=det_send.at[k - 1],
            recv_sem=det_recv.at[k - 1], device_id={"det": (det + k) % det_size}, device_id_type=MESH,
        )
        copy.start()
        copies.append(copy)
    for copy in copies:
        copy.wait()
    total = det_slots[0]
    for k in range(1, det_size):
        total = total + det_slots[k]
    total = total * scale
    place = tm % share
    own = total
    for k in range(1, share):
        own = jnp.where(place == k, pltpu.roll(total, LANES - k * (LANES // share), 1), own)
    own_ref[...] = own
    flat_out.wait()


def whole(sizes, scale, owners, inputs):
    data, templates, wafer_of, knee_freq, white_level, tile_id, pixel_id, tile_order = inputs
    x_size, z_size, det_size = sizes
    rows, local = data.shape
    dets, samples = tile_id.shape
    stored = (tile_id, pixel_id) + tables(owners)
    vmem = pl.BlockSpec(memory_space=pltpu.VMEM)
    smem = pl.BlockSpec(memory_space=pltpu.SMEM)
    anywhere = pl.BlockSpec(memory_space=pltpu.HBM)
    part = (8, LANES)
    near_size = 2 * x_size
    dma = pltpu.SemaphoreType.DMA
    return pl.pallas_call(
        functools.partial(whole_kernel, sizes, scale),
        out_shape=(
            jax.ShapeDtypeStruct((MODES, rows), f32),
            jax.ShapeDtypeStruct((dets * samples // LANES, LANES), bf16),
            jax.ShapeDtypeStruct((2, LANES), f32),
        ),
        in_specs=[smem] * 4 + [vmem] * 2 + [anywhere] * len(stored),
        out_specs=[vmem, anywhere, vmem],
        scratch_shapes=[pltpu.VMEM(a.shape, a.dtype) for a in stored]
        + [
            dma((len(stored),)),
            pltpu.VMEM((dets, samples), f32),
            pltpu.VMEM((dets, samples), f32),
            pltpu.VMEM((dets, 64, samples), f8),
            pltpu.VMEM((near_size,) + part, f32),
            pltpu.VMEM((near_size,) + part, f32),
            pltpu.VMEM((z_size,) + part, f32),
            pltpu.VMEM((near_size,) + part, f32),
            pltpu.VMEM((rows * local // LANES, LANES), f32),
            pltpu.VMEM((dets, samples // LANES, LANES), f32),
            pltpu.VMEM((dets * samples // LANES, LANES), f32),
            pltpu.VMEM((dets * samples // LANES, LANES), bf16),
            pltpu.VMEM((2, 16, LANES), f32),
            pltpu.VMEM((16, 2, LANES), f32),
            pltpu.VMEM((samples // LANES, LANES), f32),
            pltpu.VMEM((owners, 2, LANES), f32),
            pltpu.VMEM((det_size, 2, LANES), f32),
            dma((near_size - 1,)),
            dma((near_size - 1,)),
            dma((z_size - 1,)),
            dma((z_size - 1,)),
            dma((near_size - 1,)),
            dma((near_size - 1,)),
            dma((dets,)),
            dma((dets,)),
            dma,
            dma,
            dma((det_size - 1,)),
            dma((det_size - 1,)),
            dma,
        ],
        compiler_params=pltpu.CompilerParams(collective_id=0, has_side_effects=True, vmem_limit_bytes=67043328),
        name="whole",
    )(wafer_of, knee_freq, white_level, tile_order, data, templates, *stored)


def finish_kernel(flat_ref, amps_ref, maps_ref, flat_out, amps_out, sky_out, weight_out, held, come, go):
    count = come.shape[0]
    rows = held.shape[0] // count
    parts = [pl.ds(k * rows, rows) for k in range(count)]
    comes = [pltpu.make_async_copy(flat_ref.at[parts[k]], held.at[parts[k]], come.at[k]) for k in range(count)]
    goes = [pltpu.make_async_copy(held.at[parts[k]], flat_out.at[parts[k]], go.at[k]) for k in range(count)]
    for copy in comes:
        copy.start()
    amps_out[...] = amps_ref[...]
    share = sky_out.shape[1]
    sky_out[...] = maps_ref[0:1, 0:share]
    weight_out[...] = maps_ref[1:2, 0:share]
    for k in range(count):
        comes[k].wait()
        goes[k].start()
    for copy in goes:
        copy.wait()


def finish(fit_amps, flat, maps, share):
    vmem = pl.BlockSpec(memory_space=pltpu.VMEM)
    hbm = pl.BlockSpec(memory_space=pltpu.HBM)
    return pl.pallas_call(
        finish_kernel,
        out_shape=(
            jax.ShapeDtypeStruct(flat.shape, flat.dtype),
            jax.ShapeDtypeStruct(fit_amps.shape, fit_amps.dtype),
            jax.ShapeDtypeStruct((1, share), f32),
            jax.ShapeDtypeStruct((1, share), f32),
        ),
        in_specs=[hbm, vmem, vmem],
        out_specs=[hbm, vmem, vmem, vmem],
        scratch_shapes=[
            pltpu.VMEM(flat.shape, flat.dtype),
            pltpu.SemaphoreType.DMA((4,)),
            pltpu.SemaphoreType.DMA((4,)),
        ],
        compiler_params=pltpu.CompilerParams(vmem_limit_bytes=67043328),
        name="finish",
    )(flat, fit_amps, maps)


def shards(mesh, *inputs):
    owners = mesh.shape["tm"]
    det_size = mesh.shape["det"]
    dets, samples = inputs[5].shape
    cells = 16 * PIX
    scale = float(cells) / float(dets * owners * det_size * samples)
    fit_amps, flat, maps = whole((owners // 16, 8, det_size), scale, owners, inputs)
    flat, fit_amps, sky, weight = finish(fit_amps, flat, maps, cells // owners)
    weighted = flat.reshape(samples // LANES, dets, LANES).transpose(1, 0, 2).reshape(dets, samples)
    return (fit_amps, weighted, sky.reshape(-1), weight.reshape(-1))


def solution(mesh):
    in_specs = (
        P("det", "tm"),
        P(None, None, "tm"),
        P("det"),
        P(("det", "tm")),
        P(("det", "tm")),
        P(("det", "tm"), None),
        P(("det", "tm"), None),
        P(),
    )
    out_specs = (P(None, "det"), P(("det", "tm"), None), P("tm"), P("tm"))
    return jax.shard_map(
        functools.partial(shards, mesh), mesh=mesh, in_specs=in_specs, out_specs=out_specs, check_vma=False
    )
```

```python
import functools
import math

import jax
import jax.numpy as jnp
import numpy as np
from jax import lax
from jax.experimental import pallas as pl
from jax.experimental.pallas import tpu as pltpu
from jax.sharding import PartitionSpec as P

PIX = 128
MODES = 16
LANES = 128
SIDE = 256
HALF = SIDE // 2
ROWS = HALF + 8
sample_rate = 200.0
f32 = jnp.float32
bf16 = jnp.bfloat16
MESH = pl.DeviceIdType.MESH
NT = (((1,), (1,)), ((), ()))
NN = (((1,), (0,)), ((), ()))


def mm(a, b, dims=NN):
    return lax.dot_general(a, b, dims, preferred_element_type=f32)


def split2(x):
    high = x.astype(bf16)
    low = (x - high.astype(f32)).astype(bf16)
    return high, low


def split3(x):
    high = x.astype(bf16)
    rest = x - high.astype(f32)
    mid = rest.astype(bf16)
    low = (rest - mid.astype(f32)).astype(bf16)
    return high, mid, low


def tables(chunks):
    full = SIDE * SIDE
    per = SIDE // chunks
    ramp = np.arange(SIDE)
    order = np.array([per * s + j for j in range(per) for s in range(chunks)])
    angle = 2.0 * np.pi / SIDE * (np.outer(ramp, ramp) % SIDE)
    cos, sin = np.cos(angle), np.sin(angle)
    first = np.concatenate([cos[:HALF], -sin[:HALF]], axis=0)
    first[HALF] = cos[HALF]
    second = np.block([[cos, -sin], [sin, cos]])
    weight = np.full((HALF,), 2.0)
    weight[0] = 1.0
    last = np.concatenate([cos[:, :HALF] * weight, -sin[:, :HALF] * weight], axis=1)
    last[:, HALF] = cos[:, HALF]
    k = np.arange(ROWS)
    turn = 2.0 * np.pi / full * np.outer(k, ramp)
    valid = (k <= HALF)[:, None]
    turn_cos, turn_sin = np.cos(turn) * valid, np.sin(turn) * valid
    bins = k[:, None] + SIDE * ramp[None, :]
    folded = np.minimum(bins, full - bins).astype(np.float32)
    frequency = folded * np.float32(sample_rate / full)
    squared = np.where(valid, frequency * frequency, np.float32(0)).astype(np.float32)

    def halves(a):
        a = a.astype(np.float32)
        high = a.astype(jnp.bfloat16)
        return high, (a - high.astype(np.float32)).astype(jnp.bfloat16)

    return (
        *halves(first[:, order]),
        *halves(second),
        *halves(last / full),
        turn_cos.astype(np.float32),
        turn_sin.astype(np.float32),
        squared,
    )


def three(left, right, dims=NN):
    return mm(left[0], right[0], dims) + mm(left[0], right[1], dims) + mm(left[1], right[0], dims)


CHUNK = 8192
f8 = jnp.float8_e4m3fn


def whole_kernel(
    sizes, scale, wafer_ref, knee_ref, white_ref, order_ref, data_hbm, templates_ref, *refs
):
    x_size, z_size, det_size = sizes
    stored, refs = refs[:11], refs[11:]
    amps_ref, flat_ref, own_ref = refs[:3]
    held, refs = refs[3:14], refs[14:]
    (
        data_ref, load_sem, fetch_sem, left_ids, right_ids, hots, gains, parts, near_slots, z_slots, both, sent, got, flat, rounded, comb, maps_ref, rows_out,
        tm_slots, det_slots, near_send, near_recv, z_send, z_recv, back_send, back_recv, move_send, move_recv,
        tm_send, tm_recv, det_send, det_recv, flat_sem,
    ) = refs
    tile_ref, pixel_ref = held[:2]
    first_high, first_low, second_high, second_low, last_high, last_low, turn_cos, turn_sin, squared_ref = held[2:]
    dets, samples = tile_ref.shape
    owners = x_size * z_size * 2
    tm = lax.axis_index("tm")
    det = lax.axis_index("det")
    core = tm % 2
    z = (tm // 2) % z_size
    x = tm // (2 * z_size)

    def index_of(x_at, z_at, core_at):
        return (x_at * z_size + z_at) * 2 + core_at

    near_size = 2 * x_size
    near = x * 2 + core
    near_at = [(near + k) % near_size for k in range(1, near_size)]
    near_peers = [index_of(at // 2, z, at % 2) for at in near_at]
    z_peers = [index_of(x, (z + k) % z_size, core) for k in range(1, z_size)]
    peers = near_peers + z_peers
    other = near_peers[0]
    barrier = pltpu.get_barrier_semaphore()
    for peer in peers:
        pl.semaphore_signal(barrier, inc=1, device_id={"tm": peer}, device_id_type=MESH)
    for k in range(1, det_size):
        pl.semaphore_signal(barrier, inc=1, device_id={"det": (det + k) % det_size}, device_id_type=MESH)
    fetches = [
        pltpu.make_async_copy(stored[k], held[k], fetch_sem.at[k]) for k in range(len(stored))
    ]

    run = data_ref.shape[0] // 2
    loads = [
        pltpu.make_async_copy(data_hbm.at[pl.ds(w * run, run)], data_ref.at[pl.ds(w * run, run)], load_sem.at[w])
        for w in range(2)
    ]
    for load in loads:
        load.start()
    for fetch in fetches:
        fetch.start()
    shapes = []
    for w in range(2):
        loads[w].wait()
        shape = templates_ref[wafer_ref[w * run]]
        shapes.append(shape)
        high, low = split2(data_ref[w * run : (w + 1) * run, :])
        projected = mm(shape, high, NT) + mm(shape, low, NT)
        gram = mm(shape, shape, NT)
        pad = jnp.zeros((8, LANES - 2 * MODES), f32)
        parts[w * 4] = projected[0:8]
        parts[w * 4 + 1] = projected[8:16]
        parts[w * 4 + 2] = jnp.concatenate([gram[0:8], gram[8:16], pad], axis=1)
        parts[w * 4 + 3] = jnp.zeros((8, LANES), f32)

    pl.semaphore_wait(barrier, len(peers) + det_size - 1)
    near_copies = []
    for k in range(near_size - 1):
        copy = pltpu.make_async_remote_copy(
            src_ref=parts.at[near_at[k]], dst_ref=near_slots.at[near], send_sem=near_send.at[k],
            recv_sem=near_recv.at[k], device_id={"tm": near_peers[k]}, device_id_type=MESH,
        )
        copy.start()
        near_copies.append(copy)
    near_slots[near] = parts[near]

    def ids(turn, carry):
        span = pl.ds(pl.multiple_of(turn * CHUNK, CHUNK), CHUNK)
        tiles = tile_ref[:, span]
        pixels = pixel_ref[:, span]
        left_ids[:, span] = (tiles + 16 * (pixels >> 6)).astype(f32)
        right_ids[:, span] = (pixels & 63).astype(f32)
        return carry

    for fetch in fetches[:2]:
        fetch.wait()
    lax.fori_loop(0, samples // CHUNK, ids, 0)
    one, zero = jnp.ones((), bf16), jnp.zeros((), bf16)

    def ramp(rows):
        return lax.broadcasted_iota(jnp.int32, (rows, CHUNK), 0).astype(f32).astype(bf16)

    def left_hot(d, span, value):
        left_id = left_ids[pl.ds(d, 1), span].astype(bf16)
        return jnp.where(left_id == ramp(32), value, zero)

    def count(d, total):
        def step(turn, total):
            span = pl.ds(pl.multiple_of(turn * CHUNK, CHUNK), CHUNK)
            right_id = right_ids[pl.ds(d, 1), span].astype(bf16)
            right = jnp.where(right_id == ramp(64), one, zero).astype(f8)
            hots[d, :, span] = right
            return total + mm(left_hot(d, span, one), right, NT)

        inverse = (jnp.ones((1, 64), f32) / jnp.full((1, 64), white_ref[d], f32)).astype(bf16).astype(f32)
        return total + lax.fori_loop(0, samples // CHUNK, step, jnp.zeros((32, 64), f32)) * inverse

    def spread(slots, place, peers, send_sem, recv_sem):
        copies = []
        for k, peer in enumerate(peers):
            copy = pltpu.make_async_remote_copy(
                src_ref=slots.at[place], dst_ref=slots.at[place], send_sem=send_sem.at[k], recv_sem=recv_sem.at[k],
                device_id={"tm": peer}, device_id_type=MESH,
            )
            copy.start()
            copies.append(copy)
        return copies

    def gathered(slots, copies):
        for copy in copies:
            copy.wait()
        total = slots[0]
        for k in range(1, len(copies) + 1):
            total = total + slots[k]
        return total

    weight = count(0, jnp.zeros((32, 64), f32))
    z_slots[z] = gathered(near_slots, near_copies)
    copies = spread(z_slots, z, z_peers, z_send, z_recv)
    weight = count(1, weight)
    both[near] = gathered(z_slots, copies)
    copies = spread(both, near, near_peers, back_send, back_recv)
    for copy in copies:
        copy.wait()

    row = lax.broadcasted_iota(jnp.int32, (1, MODES, LANES), 1)
    for w in range(2):
        packed = both[w * 4 + 2]
        columns = []
        for k in range(MODES):
            top = jnp.broadcast_to(packed[:, k : k + 1], (8, LANES))
            low = jnp.broadcast_to(packed[:, MODES + k : MODES + k + 1], (8, LANES))
            columns.append(jnp.concatenate([top, low], axis=0))
        columns.append(jnp.concatenate([both[w * 4], both[w * 4 + 1]], axis=0))
        joined = jnp.stack(columns, axis=0)
        for c in range(MODES):
            factor = joined[0:1]
            pivot_row = joined[1:, c : c + 1, :] / factor[:, c : c + 1, :]
            joined = jnp.where(row == c, pivot_row, joined[1:] - factor * pivot_row)
        amps = joined[0]
        amps_ref[:, w * run : (w + 1) * run] = amps
        high, mid, low = split3(amps)
        left = jnp.concatenate([high, mid, low], axis=0)
        right = jnp.concatenate([shapes[w]] * 3, axis=0)
        fitted = lax.dot_general(left, right, (((0,), (0,)), ((), ())), preferred_element_type=f32)
        residual = data_ref[w * run : (w + 1) * run, :] - fitted
        tiles = residual.shape[1] // LANES
        for l in range(tiles):
            sent[pl.ds(w * run * tiles + l, run, stride=tiles), :] = residual[:, l * LANES : (l + 1) * LANES]

    piece = got.shape[1] // owners

    def move(d, carry):
        def one_peer(k, carry):
            peer = (tm + k) % owners
            pltpu.make_async_remote_copy(
                src_ref=sent.at[pl.ds((peer * dets + d) * piece, piece)], dst_ref=got.at[d, pl.ds(tm * piece, piece)],
                send_sem=move_send.at[d], recv_sem=move_recv.at[d], device_id={"tm": peer}, device_id_type=MESH,
            ).start()
            return carry

        lax.fori_loop(1, owners, one_peer, 0)
        got[d, pl.ds(pl.multiple_of(tm * piece, piece), piece), :] = sent[
            pl.ds(pl.multiple_of((tm * dets + d) * piece, piece), piece), :
        ]
        return carry

    lax.fori_loop(0, dets, move, 0)
    weight = lax.fori_loop(2, dets, count, weight)
    for fetch in fetches[2:]:
        fetch.wait()

    def gain_of(d, carry):
        squared = squared_ref[...]
        knee = knee_ref[d]
        gains[d] = squared / (white_ref[d] * (squared + knee * knee))
        return carry

    lax.fori_loop(0, dets, gain_of, 0)
    chunks = owners
    per = SIDE // chunks
    tiles = SIDE // LANES

    def turned(ref):
        upper = jnp.concatenate([ref[0:SIDE, 0:SIDE], ref[SIDE:, 0:SIDE]], axis=1)
        lower = jnp.concatenate([ref[0:SIDE, SIDE:], ref[SIDE:, SIDE:]], axis=1)
        return jnp.concatenate([upper, lower], axis=0)

    def weigh(d, total):
        arrived = pltpu.make_async_remote_copy(
            src_ref=got.at[d, pl.ds(0, (owners - 1) * piece)], dst_ref=got.at[d, pl.ds(0, (owners - 1) * piece)],
            send_sem=move_send.at[d], recv_sem=move_recv.at[d], device_id={"tm": other}, device_id_type=MESH,
        )
        arrived.wait()
        rows = []
        for j in range(per):
            rows.append(
                jnp.concatenate(
                    [got[d, pl.ds(j * tiles + h, chunks, stride=piece), :] for h in range(tiles)], axis=1
                )
            )
        signal = jnp.concatenate(rows, axis=0)
        spectrum = three((first_high[...], first_low[...]), split2(signal))
        real_y, imag_y, tail = spectrum[0:HALF], spectrum[HALF:], spectrum[HALF : HALF + 8]
        first_row = lax.broadcasted_iota(jnp.int32, (HALF, SIDE), 0) == 0
        imag_y = jnp.where(first_row, 0.0, imag_y)
        cos_main, sin_main = turn_cos[0:HALF, :], turn_sin[0:HALF, :]
        cos_tail, sin_tail = turn_cos[HALF:, :], turn_sin[HALF:, :]
        real_z = jnp.concatenate([real_y * cos_main + imag_y * sin_main, tail * cos_tail], axis=0)
        imag_z = jnp.concatenate([imag_y * cos_main - real_y * sin_main, -tail * sin_tail], axis=0)
        bins = three(
            split2(jnp.concatenate([real_z, imag_z], axis=1)), (second_high[...], second_low[...])
        )
        gain = gains[d]
        bins = bins * jnp.concatenate([gain, gain], axis=1)
        back = three(split2(bins), (turned(second_high), turned(second_low)))
        real_u, imag_u = back[:, 0:SIDE], back[:, SIDE:]
        real_w = real_u[0:HALF] * cos_main - imag_u[0:HALF] * sin_main
        imag_w = real_u[0:HALF] * sin_main + imag_u[0:HALF] * cos_main
        tail_w = (real_u[HALF:] * cos_tail - imag_u[HALF:] * sin_tail)[0:1]
        imag_w = jnp.where(first_row, jnp.broadcast_to(tail_w, (HALF, SIDE)), imag_w)
        joined = jnp.concatenate([real_w, imag_w], axis=0)
        output = three((last_high[...], last_low[...]), split2(joined))
        for h in range(tiles):
            part = output[:, h * LANES : (h + 1) * LANES]
            flat[pl.ds(h * dets + d, SIDE, stride=tiles * dets), :] = part
            rows_out[pl.ds(h, SIDE, stride=tiles), :] = part.astype(bf16).astype(f32)

        def step(turn, total):
            span = pl.ds(pl.multiple_of(turn * CHUNK, CHUNK), CHUNK)
            width = CHUNK // LANES
            values = rows_out[pl.ds(pl.multiple_of(turn * width, width), width), :].astype(bf16)
            value = jnp.concatenate([values[l : l + 1, :] for l in range(width)], axis=1)
            return total + mm(left_hot(d, span, value), hots[d, :, span], NT)

        return lax.fori_loop(0, samples // CHUNK, step, total)

    sky = lax.fori_loop(0, dets, weigh, jnp.zeros((32, 64), f32))
    comb[0] = jnp.concatenate([sky[0:16], sky[16:32]], axis=1)
    comb[1] = jnp.concatenate([weight[0:16], weight[16:32]], axis=1)
    share = owners // 16
    ordered = maps_ref.shape[0]
    for r in range(ordered):
        tile = order_ref[r]
        maps_ref[r, 0:1, :] = comb[0, pl.ds(tile, 1), :]
        maps_ref[r, 1:2, :] = comb[1, pl.ds(tile, 1), :]

    def send(dx, dz, dc):
        peer = index_of((x + dx) % x_size, (z + dz) % z_size, (core + dc) % 2)
        pltpu.make_async_remote_copy(
            src_ref=maps_ref.at[peer // share], dst_ref=tm_slots.at[tm], send_sem=tm_send, recv_sem=tm_recv,
            device_id={"tm": peer}, device_id_type=MESH,
        ).start()

    def far_first(size):
        return sorted(range(size), key=lambda k: -min(k, size - k))

    near_steps = [(dx, dc) for dx in far_first(x_size) for dc in (1, 0)]

    def send_far(j, carry):
        dz = z_size // 2 + (j + 1) // 2 * (2 * ((j + 1) % 2) - 1)
        for dx, dc in near_steps:
            send(dx, dz, dc)
        return carry

    lax.fori_loop(0, z_size - 1, send_far, 0)
    for dx, dc in near_steps:
        if (dx, dc) != (0, 0):
            send(dx, 0, dc)
    tm_slots[tm] = maps_ref[tm // share]
    rounded[...] = flat[...].astype(bf16)
    flat_out = pltpu.make_async_copy(rounded, flat_ref, flat_sem)
    flat_out.start()
    pltpu.make_async_remote_copy(
        src_ref=tm_slots.at[pl.ds(0, owners - 1)], dst_ref=tm_slots.at[pl.ds(0, owners - 1)],
        send_sem=tm_send, recv_sem=tm_recv, device_id={"tm": other}, device_id_type=MESH,
    ).wait()
    det_slots[det] = jnp.sum(tm_slots[...], axis=0)
    copies = []
    for k in range(1, det_size):
        copy = pltpu.make_async_remote_copy(
            src_ref=det_slots.at[det], dst_ref=det_slots.at[det], send_sem=det_send.at[k - 1],
            recv_sem=det_recv.at[k - 1], device_id={"det": (det + k) % det_size}, device_id_type=MESH,
        )
        copy.start()
        copies.append(copy)
    for copy in copies:
        copy.wait()
    total = det_slots[0]
    for k in range(1, det_size):
        total = total + det_slots[k]
    total = total * scale
    place = tm % share
    own = total
    for k in range(1, share):
        own = jnp.where(place == k, pltpu.roll(total, LANES - k * (LANES // share), 1), own)
    own_ref[...] = own
    flat_out.wait()


def whole(sizes, scale, owners, inputs):
    data, templates, wafer_of, knee_freq, white_level, tile_id, pixel_id, tile_order = inputs
    x_size, z_size, det_size = sizes
    rows, local = data.shape
    dets, samples = tile_id.shape
    stored = (tile_id, pixel_id) + tables(owners)
    vmem = pl.BlockSpec(memory_space=pltpu.VMEM)
    smem = pl.BlockSpec(memory_space=pltpu.SMEM)
    anywhere = pl.BlockSpec(memory_space=pltpu.HBM)
    part = (8, LANES)
    near_size = 2 * x_size
    dma = pltpu.SemaphoreType.DMA
    return pl.pallas_call(
        functools.partial(whole_kernel, sizes, scale),
        out_shape=(
            jax.ShapeDtypeStruct((MODES, rows), f32),
            jax.ShapeDtypeStruct((dets * samples // LANES, LANES), bf16),
            jax.ShapeDtypeStruct((2, LANES), f32),
        ),
        in_specs=[smem] * 4 + [anywhere, vmem] + [anywhere] * len(stored),
        out_specs=[vmem, anywhere, vmem],
        scratch_shapes=[pltpu.VMEM(a.shape, a.dtype) for a in stored]
        + [
            pltpu.VMEM(data.shape, f32),
            dma((2,)),
            dma((len(stored),)),
            pltpu.VMEM((dets, samples), f32),
            pltpu.VMEM((dets, samples), f32),
            pltpu.VMEM((dets, 64, samples), f8),
            pltpu.VMEM((dets, ROWS, SIDE), f32),
            pltpu.VMEM((near_size,) + part, f32),
            pltpu.VMEM((near_size,) + part, f32),
            pltpu.VMEM((z_size,) + part, f32),
            pltpu.VMEM((near_size,) + part, f32),
            pltpu.VMEM((rows * local // LANES, LANES), f32),
            pltpu.VMEM((dets, samples // LANES, LANES), f32),
            pltpu.VMEM((dets * samples // LANES, LANES), f32),
            pltpu.VMEM((dets * samples // LANES, LANES), bf16),
            pltpu.VMEM((2, 16, LANES), f32),
            pltpu.VMEM((16, 2, LANES), f32),
            pltpu.VMEM((samples // LANES, LANES), f32),
            pltpu.VMEM((owners, 2, LANES), f32),
            pltpu.VMEM((det_size, 2, LANES), f32),
            dma((near_size - 1,)),
            dma((near_size - 1,)),
            dma((z_size - 1,)),
            dma((z_size - 1,)),
            dma((near_size - 1,)),
            dma((near_size - 1,)),
            dma((dets,)),
            dma((dets,)),
            dma,
            dma,
            dma((det_size - 1,)),
            dma((det_size - 1,)),
            dma,
        ],
        compiler_params=pltpu.CompilerParams(collective_id=0, has_side_effects=True, vmem_limit_bytes=67043328),
        name="whole",
    )(wafer_of, knee_freq, white_level, tile_order, data, templates, *stored)


def finish_kernel(
    flat_ref, amps_ref, own_ref, flat_out, amps_out, sky_out, weight_out, held, amps, own, sky, weight, come, go
):
    parts = come.shape[0] - 2
    rows = held.shape[0] // parts
    cuts = [pl.ds(k * rows, rows) for k in range(parts)]
    comes = [pltpu.make_async_copy(own_ref, own, come.at[parts]), pltpu.make_async_copy(amps_ref, amps, come.at[parts + 1])]
    comes += [pltpu.make_async_copy(flat_ref.at[cuts[k]], held.at[cuts[k]], come.at[k]) for k in range(parts)]
    goes = [pltpu.make_async_copy(held.at[cuts[k]], flat_out.at[cuts[k]], go.at[k]) for k in range(parts)]
    for copy in comes:
        copy.start()
    comes[0].wait()
    share = sky.shape[1]
    sky[...] = own[0:1, 0:share]
    weight[...] = own[1:2, 0:share]
    goes.append(pltpu.make_async_copy(sky, sky_out, go.at[parts]))
    goes.append(pltpu.make_async_copy(weight, weight_out, go.at[parts + 1]))
    for copy in goes[parts:]:
        copy.start()
    comes[1].wait()
    goes.append(pltpu.make_async_copy(amps, amps_out, go.at[parts + 2]))
    goes[-1].start()
    for k in range(parts):
        comes[2 + k].wait()
        goes[k].start()
    for copy in goes:
        copy.wait()


def finish(fit_amps, flat, own, share):
    hbm = pl.BlockSpec(memory_space=pltpu.HBM)
    parts = 4
    return pl.pallas_call(
        finish_kernel,
        out_shape=(
            jax.ShapeDtypeStruct(flat.shape, flat.dtype),
            jax.ShapeDtypeStruct(fit_amps.shape, fit_amps.dtype),
            jax.ShapeDtypeStruct((1, share), f32),
            jax.ShapeDtypeStruct((1, share), f32),
        ),
        in_specs=[hbm] * 3,
        out_specs=[hbm] * 4,
        scratch_shapes=[
            pltpu.VMEM(flat.shape, flat.dtype),
            pltpu.VMEM(fit_amps.shape, f32),
            pltpu.VMEM(own.shape, f32),
            pltpu.VMEM((1, share), f32),
            pltpu.VMEM((1, share), f32),
            pltpu.SemaphoreType.DMA((parts + 2,)),
            pltpu.SemaphoreType.DMA((parts + 3,)),
        ],
        compiler_params=pltpu.CompilerParams(vmem_limit_bytes=67043328),
        name="finish",
    )(flat, fit_amps, own)


def shards(mesh, *inputs):
    owners = mesh.shape["tm"]
    det_size = mesh.shape["det"]
    dets, samples = inputs[5].shape
    cells = 16 * PIX
    scale = float(cells) / float(dets * owners * det_size * samples)
    fit_amps, flat, maps = whole((owners // 16, 8, det_size), scale, owners, inputs)
    flat, fit_amps, sky, weight = finish(fit_amps, flat, maps, cells // owners)
    weighted = flat.reshape(samples // LANES, dets, LANES).transpose(1, 0, 2).reshape(dets, samples)
    return (fit_amps, weighted, sky.reshape(-1), weight.reshape(-1))


def solution(mesh):
    in_specs = (
        P("det", "tm"),
        P(None, None, "tm"),
        P("det"),
        P(("det", "tm")),
        P(("det", "tm")),
        P(("det", "tm"), None),
        P(("det", "tm"), None),
        P(),
    )
    out_specs = (P(None, "det"), P(("det", "tm"), None), P("tm"), P("tm"))
    return jax.shard_map(
        functools.partial(shards, mesh), mesh=mesh, in_specs=in_specs, out_specs=out_specs, check_vma=False
    )
```

```python
import functools
import math

import jax
import jax.numpy as jnp
import numpy as np
from jax import lax
from jax.experimental import pallas as pl
from jax.experimental.pallas import tpu as pltpu
from jax.sharding import PartitionSpec as P

PIX = 128
MODES = 16
LANES = 128
SIDE = 256
HALF = SIDE // 2
ROWS = HALF + 8
sample_rate = 200.0
f32 = jnp.float32
bf16 = jnp.bfloat16
MESH = pl.DeviceIdType.MESH
NT = (((1,), (1,)), ((), ()))
NN = (((1,), (0,)), ((), ()))


def mm(a, b, dims=NN):
    return lax.dot_general(a, b, dims, preferred_element_type=f32)


def split2(x):
    high = x.astype(bf16)
    low = (x - high.astype(f32)).astype(bf16)
    return high, low


def split3(x):
    high = x.astype(bf16)
    rest = x - high.astype(f32)
    mid = rest.astype(bf16)
    low = (rest - mid.astype(f32)).astype(bf16)
    return high, mid, low


def tables(chunks):
    full = SIDE * SIDE
    per = SIDE // chunks
    ramp = np.arange(SIDE)
    order = np.array([per * s + j for j in range(per) for s in range(chunks)])
    angle = 2.0 * np.pi / SIDE * (np.outer(ramp, ramp) % SIDE)
    cos, sin = np.cos(angle), np.sin(angle)
    first = np.concatenate([cos[:HALF], -sin[:HALF]], axis=0)
    first[HALF] = cos[HALF]
    second = np.block([[cos, -sin], [sin, cos]])
    weight = np.full((HALF,), 2.0)
    weight[0] = 1.0
    last = np.concatenate([cos[:, :HALF] * weight, -sin[:, :HALF] * weight], axis=1)
    last[:, HALF] = cos[:, HALF]
    k = np.arange(ROWS)
    turn = 2.0 * np.pi / full * np.outer(k, ramp)
    valid = (k <= HALF)[:, None]
    turn_cos, turn_sin = np.cos(turn) * valid, np.sin(turn) * valid
    bins = k[:, None] + SIDE * ramp[None, :]
    folded = np.minimum(bins, full - bins).astype(np.float32)
    frequency = folded * np.float32(sample_rate / full)
    squared = np.where(valid, frequency * frequency, np.float32(0)).astype(np.float32)

    def halves(a):
        a = a.astype(np.float32)
        high = a.astype(jnp.bfloat16)
        return high, (a - high.astype(np.float32)).astype(jnp.bfloat16)

    return (
        *halves(first[:, order]),
        *halves(second),
        *halves(last / full),
        turn_cos.astype(np.float32),
        turn_sin.astype(np.float32),
        squared,
    )


def three(left, right, dims=NN):
    return mm(left[0], right[0], dims) + mm(left[0], right[1], dims) + mm(left[1], right[0], dims)


CHUNK = 16384
f8 = jnp.float8_e4m3fn


def whole_kernel(
    sizes, scale, wafer_ref, knee_ref, white_ref, order_ref, data_hbm, templates_ref, *refs
):
    x_size, z_size, det_size = sizes
    stored, refs = refs[:11], refs[11:]
    amps_ref, flat_ref, own_ref = refs[:3]
    held, refs = refs[3:14], refs[14:]
    (
        data_ref, load_sem, fetch_sem, left_ids, right_ids, hots, gains, parts, near_slots, z_slots, both, sent, got, flat, rounded, comb, maps_ref, rows_out,
        tm_slots, det_slots, near_send, near_recv, z_send, z_recv, back_send, back_recv, move_send, move_recv,
        tm_send, tm_recv, det_send, det_recv, flat_sem,
    ) = refs
    tile_ref, pixel_ref = held[:2]
    first_high, first_low, second_high, second_low, last_high, last_low, turn_cos, turn_sin, squared_ref = held[2:]
    dets, samples = tile_ref.shape
    owners = x_size * z_size * 2
    tm = lax.axis_index("tm")
    det = lax.axis_index("det")
    core = tm % 2
    z = (tm // 2) % z_size
    x = tm // (2 * z_size)

    def index_of(x_at, z_at, core_at):
        return (x_at * z_size + z_at) * 2 + core_at

    near_size = 2 * x_size
    near = x * 2 + core
    near_at = [(near + k) % near_size for k in range(1, near_size)]
    near_peers = [index_of(at // 2, z, at % 2) for at in near_at]
    z_peers = [index_of(x, (z + k) % z_size, core) for k in range(1, z_size)]
    peers = near_peers + z_peers
    other = near_peers[0]
    barrier = pltpu.get_barrier_semaphore()
    for peer in peers:
        pl.semaphore_signal(barrier, inc=1, device_id={"tm": peer}, device_id_type=MESH)
    for k in range(1, det_size):
        pl.semaphore_signal(barrier, inc=1, device_id={"det": (det + k) % det_size}, device_id_type=MESH)
    fetches = [
        pltpu.make_async_copy(stored[k], held[k], fetch_sem.at[k]) for k in range(len(stored))
    ]

    run = data_ref.shape[0] // 2
    loads = [
        pltpu.make_async_copy(data_hbm.at[pl.ds(w * run, run)], data_ref.at[pl.ds(w * run, run)], load_sem.at[w])
        for w in range(2)
    ]
    for load in loads:
        load.start()
    for fetch in fetches:
        fetch.start()
    shapes = []
    for w in range(2):
        loads[w].wait()
        shape = templates_ref[wafer_ref[w * run]]
        shapes.append(shape)
        high, low = split2(data_ref[w * run : (w + 1) * run, :])
        projected = mm(shape, high, NT) + mm(shape, low, NT)
        gram = mm(shape, shape, NT)
        pad = jnp.zeros((8, LANES - 2 * MODES), f32)
        parts[w * 4] = projected[0:8]
        parts[w * 4 + 1] = projected[8:16]
        parts[w * 4 + 2] = jnp.concatenate([gram[0:8], gram[8:16], pad], axis=1)
        parts[w * 4 + 3] = jnp.zeros((8, LANES), f32)

    pl.semaphore_wait(barrier, len(peers) + det_size - 1)
    near_copies = []
    for k in range(near_size - 1):
        copy = pltpu.make_async_remote_copy(
            src_ref=parts.at[near_at[k]], dst_ref=near_slots.at[near], send_sem=near_send.at[k],
            recv_sem=near_recv.at[k], device_id={"tm": near_peers[k]}, device_id_type=MESH,
        )
        copy.start()
        near_copies.append(copy)
    near_slots[near] = parts[near]

    def ids(turn, carry):
        span = pl.ds(pl.multiple_of(turn * CHUNK, CHUNK), CHUNK)
        tiles = tile_ref[:, span]
        pixels = pixel_ref[:, span]
        left_ids[:, span] = (tiles + 16 * (pixels >> 6)).astype(f32)
        right_ids[:, span] = (pixels & 63).astype(f32)
        return carry

    for fetch in fetches[:2]:
        fetch.wait()
    lax.fori_loop(0, samples // CHUNK, ids, 0)
    one, zero = jnp.ones((), bf16), jnp.zeros((), bf16)

    def ramp(rows):
        return lax.broadcasted_iota(jnp.int32, (rows, CHUNK), 0).astype(f32).astype(bf16)

    def left_hot(d, span, value):
        left_id = left_ids[pl.ds(d, 1), span].astype(bf16)
        return jnp.where(left_id == ramp(32), value, zero)

    def count(d, total):
        def step(turn, total):
            span = pl.ds(pl.multiple_of(turn * CHUNK, CHUNK), CHUNK)
            right_id = right_ids[pl.ds(d, 1), span].astype(bf16)
            right = jnp.where(right_id == ramp(64), one, zero).astype(f8)
            hots[d, :, span] = right
            return total + mm(left_hot(d, span, one), right, NT)

        inverse = (jnp.ones((1, 64), f32) / jnp.full((1, 64), white_ref[d], f32)).astype(bf16).astype(f32)
        return total + lax.fori_loop(0, samples // CHUNK, step, jnp.zeros((32, 64), f32)) * inverse

    def spread(slots, place, peers, send_sem, recv_sem):
        copies = []
        for k, peer in enumerate(peers):
            copy = pltpu.make_async_remote_copy(
                src_ref=slots.at[place], dst_ref=slots.at[place], send_sem=send_sem.at[k], recv_sem=recv_sem.at[k],
                device_id={"tm": peer}, device_id_type=MESH,
            )
            copy.start()
            copies.append(copy)
        return copies

    def gathered(slots, copies):
        for copy in copies:
            copy.wait()
        total = slots[0]
        for k in range(1, len(copies) + 1):
            total = total + slots[k]
        return total

    weight = count(0, jnp.zeros((32, 64), f32))
    z_slots[z] = gathered(near_slots, near_copies)
    copies = spread(z_slots, z, z_peers, z_send, z_recv)
    weight = count(1, weight)
    both[near] = gathered(z_slots, copies)
    copies = spread(both, near, near_peers, back_send, back_recv)
    for copy in copies:
        copy.wait()

    row = lax.broadcasted_iota(jnp.int32, (1, MODES, LANES), 1)
    for w in range(2):
        packed = both[w * 4 + 2]
        columns = []
        for k in range(MODES):
            top = jnp.broadcast_to(packed[:, k : k + 1], (8, LANES))
            low = jnp.broadcast_to(packed[:, MODES + k : MODES + k + 1], (8, LANES))
            columns.append(jnp.concatenate([top, low], axis=0))
        columns.append(jnp.concatenate([both[w * 4], both[w * 4 + 1]], axis=0))
        joined = jnp.stack(columns, axis=0)
        for c in range(MODES):
            factor = joined[0:1]
            pivot_row = joined[1:, c : c + 1, :] / factor[:, c : c + 1, :]
            joined = jnp.where(row == c, pivot_row, joined[1:] - factor * pivot_row)
        amps = joined[0]
        amps_ref[:, w * run : (w + 1) * run] = amps
        high, mid, low = split3(amps)
        left = jnp.concatenate([high, mid, low], axis=0)
        right = jnp.concatenate([shapes[w]] * 3, axis=0)
        fitted = lax.dot_general(left, right, (((0,), (0,)), ((), ())), preferred_element_type=f32)
        residual = data_ref[w * run : (w + 1) * run, :] - fitted
        tiles = residual.shape[1] // LANES
        for l in range(tiles):
            sent[pl.ds(w * run * tiles + l, run, stride=tiles), :] = residual[:, l * LANES : (l + 1) * LANES]

    piece = got.shape[1] // owners

    def move(d, carry):
        def one_peer(k, carry):
            peer = (tm + k) % owners
            pltpu.make_async_remote_copy(
                src_ref=sent.at[pl.ds((peer * dets + d) * piece, piece)], dst_ref=got.at[d, pl.ds(tm * piece, piece)],
                send_sem=move_send.at[d], recv_sem=move_recv.at[d], device_id={"tm": peer}, device_id_type=MESH,
            ).start()
            return carry

        lax.fori_loop(1, owners, one_peer, 0)
        got[d, pl.ds(pl.multiple_of(tm * piece, piece), piece), :] = sent[
            pl.ds(pl.multiple_of((tm * dets + d) * piece, piece), piece), :
        ]
        return carry

    lax.fori_loop(0, dets, move, 0)
    weight = lax.fori_loop(2, dets, count, weight)
    for fetch in fetches[2:]:
        fetch.wait()

    def gain_of(d, carry):
        squared = squared_ref[...]
        knee = knee_ref[d]
        gains[d] = squared / (white_ref[d] * (squared + knee * knee))
        return carry

    lax.fori_loop(0, dets, gain_of, 0)
    chunks = owners
    per = SIDE // chunks
    tiles = SIDE // LANES

    def turned(ref):
        upper = jnp.concatenate([ref[0:SIDE, 0:SIDE], ref[SIDE:, 0:SIDE]], axis=1)
        lower = jnp.concatenate([ref[0:SIDE, SIDE:], ref[SIDE:, SIDE:]], axis=1)
        return jnp.concatenate([upper, lower], axis=0)

    def weigh(d, total):
        arrived = pltpu.make_async_remote_copy(
            src_ref=got.at[d, pl.ds(0, (owners - 1) * piece)], dst_ref=got.at[d, pl.ds(0, (owners - 1) * piece)],
            send_sem=move_send.at[d], recv_sem=move_recv.at[d], device_id={"tm": other}, device_id_type=MESH,
        )
        arrived.wait()
        rows = []
        for j in range(per):
            rows.append(
                jnp.concatenate(
                    [got[d, pl.ds(j * tiles + h, chunks, stride=piece), :] for h in range(tiles)], axis=1
                )
            )
        signal = jnp.concatenate(rows, axis=0)
        spectrum = three((first_high[...], first_low[...]), split2(signal))
        real_y, imag_y, tail = spectrum[0:HALF], spectrum[HALF:], spectrum[HALF : HALF + 8]
        first_row = lax.broadcasted_iota(jnp.int32, (HALF, SIDE), 0) == 0
        imag_y = jnp.where(first_row, 0.0, imag_y)
        cos_main, sin_main = turn_cos[0:HALF, :], turn_sin[0:HALF, :]
        cos_tail, sin_tail = turn_cos[HALF:, :], turn_sin[HALF:, :]
        real_z = jnp.concatenate([real_y * cos_main + imag_y * sin_main, tail * cos_tail], axis=0)
        imag_z = jnp.concatenate([imag_y * cos_main - real_y * sin_main, -tail * sin_tail], axis=0)
        bins = three(
            split2(jnp.concatenate([real_z, imag_z], axis=1)), (second_high[...], second_low[...])
        )
        gain = gains[d]
        bins = bins * jnp.concatenate([gain, gain], axis=1)
        back = three(split2(bins), (turned(second_high), turned(second_low)))
        real_u, imag_u = back[:, 0:SIDE], back[:, SIDE:]
        real_w = real_u[0:HALF] * cos_main - imag_u[0:HALF] * sin_main
        imag_w = real_u[0:HALF] * sin_main + imag_u[0:HALF] * cos_main
        tail_w = (real_u[HALF:] * cos_tail - imag_u[HALF:] * sin_tail)[0:1]
        imag_w = jnp.where(first_row, jnp.broadcast_to(tail_w, (HALF, SIDE)), imag_w)
        joined = jnp.concatenate([real_w, imag_w], axis=0)
        output = three((last_high[...], last_low[...]), split2(joined))
        for h in range(tiles):
            part = output[:, h * LANES : (h + 1) * LANES]
            flat[pl.ds(h * dets + d, SIDE, stride=tiles * dets), :] = part
            rows_out[pl.ds(h, SIDE, stride=tiles), :] = part.astype(bf16).astype(f32)

        def step(turn, total):
            span = pl.ds(pl.multiple_of(turn * CHUNK, CHUNK), CHUNK)
            width = CHUNK // LANES
            values = rows_out[pl.ds(pl.multiple_of(turn * width, width), width), :].astype(bf16)
            value = jnp.concatenate([values[l : l + 1, :] for l in range(width)], axis=1)
            return total + mm(left_hot(d, span, value), hots[d, :, span], NT)

        return lax.fori_loop(0, samples // CHUNK, step, total)

    sky = lax.fori_loop(0, dets, weigh, jnp.zeros((32, 64), f32))
    comb[0] = jnp.concatenate([sky[0:16], sky[16:32]], axis=1)
    comb[1] = jnp.concatenate([weight[0:16], weight[16:32]], axis=1)
    share = owners // 16
    ordered = maps_ref.shape[0]
    for r in range(ordered):
        tile = order_ref[r]
        maps_ref[r, 0:1, :] = comb[0, pl.ds(tile, 1), :]
        maps_ref[r, 1:2, :] = comb[1, pl.ds(tile, 1), :]

    def send(dx, dz, dc):
        peer = index_of((x + dx) % x_size, (z + dz) % z_size, (core + dc) % 2)
        pltpu.make_async_remote_copy(
            src_ref=maps_ref.at[peer // share], dst_ref=tm_slots.at[tm], send_sem=tm_send, recv_sem=tm_recv,
            device_id={"tm": peer}, device_id_type=MESH,
        ).start()

    def far_first(size):
        return sorted(range(size), key=lambda k: -min(k, size - k))

    near_steps = [(dx, dc) for dx in far_first(x_size) for dc in (1, 0)]

    def send_far(j, carry):
        dz = z_size // 2 + (j + 1) // 2 * (2 * ((j + 1) % 2) - 1)
        for dx, dc in near_steps:
            send(dx, dz, dc)
        return carry

    lax.fori_loop(0, z_size - 1, send_far, 0)
    for dx, dc in near_steps:
        if (dx, dc) != (0, 0):
            send(dx, 0, dc)
    tm_slots[tm] = maps_ref[tm // share]
    rounded[...] = flat[...].astype(bf16)
    flat_out = pltpu.make_async_copy(rounded, flat_ref, flat_sem)
    flat_out.start()
    pltpu.make_async_remote_copy(
        src_ref=tm_slots.at[pl.ds(0, owners - 1)], dst_ref=tm_slots.at[pl.ds(0, owners - 1)],
        send_sem=tm_send, recv_sem=tm_recv, device_id={"tm": other}, device_id_type=MESH,
    ).wait()
    det_slots[det] = jnp.sum(tm_slots[...], axis=0)
    copies = []
    for k in range(1, det_size):
        copy = pltpu.make_async_remote_copy(
            src_ref=det_slots.at[det], dst_ref=det_slots.at[det], send_sem=det_send.at[k - 1],
            recv_sem=det_recv.at[k - 1], device_id={"det": (det + k) % det_size}, device_id_type=MESH,
        )
        copy.start()
        copies.append(copy)
    for copy in copies:
        copy.wait()
    total = det_slots[0]
    for k in range(1, det_size):
        total = total + det_slots[k]
    total = total * scale
    place = tm % share
    own = total
    for k in range(1, share):
        own = jnp.where(place == k, pltpu.roll(total, LANES - k * (LANES // share), 1), own)
    own_ref[...] = own
    flat_out.wait()


def whole(sizes, scale, owners, inputs):
    data, templates, wafer_of, knee_freq, white_level, tile_id, pixel_id, tile_order = inputs
    x_size, z_size, det_size = sizes
    rows, local = data.shape
    dets, samples = tile_id.shape
    stored = (tile_id, pixel_id) + tables(owners)
    vmem = pl.BlockSpec(memory_space=pltpu.VMEM)
    smem = pl.BlockSpec(memory_space=pltpu.SMEM)
    anywhere = pl.BlockSpec(memory_space=pltpu.HBM)
    part = (8, LANES)
    near_size = 2 * x_size
    dma = pltpu.SemaphoreType.DMA
    return pl.pallas_call(
        functools.partial(whole_kernel, sizes, scale),
        out_shape=(
            jax.ShapeDtypeStruct((MODES, rows), f32),
            jax.ShapeDtypeStruct((dets * samples // LANES, LANES), bf16),
            jax.ShapeDtypeStruct((2, LANES), f32),
        ),
        in_specs=[smem] * 4 + [anywhere, vmem] + [anywhere] * len(stored),
        out_specs=[vmem, anywhere, vmem],
        scratch_shapes=[pltpu.VMEM(a.shape, a.dtype) for a in stored]
        + [
            pltpu.VMEM(data.shape, f32),
            dma((2,)),
            dma((len(stored),)),
            pltpu.VMEM((dets, samples), f32),
            pltpu.VMEM((dets, samples), f32),
            pltpu.VMEM((dets, 64, samples), f8),
            pltpu.VMEM((dets, ROWS, SIDE), f32),
            pltpu.VMEM((near_size,) + part, f32),
            pltpu.VMEM((near_size,) + part, f32),
            pltpu.VMEM((z_size,) + part, f32),
            pltpu.VMEM((near_size,) + part, f32),
            pltpu.VMEM((rows * local // LANES, LANES), f32),
            pltpu.VMEM((dets, samples // LANES, LANES), f32),
            pltpu.VMEM((dets * samples // LANES, LANES), f32),
            pltpu.VMEM((dets * samples // LANES, LANES), bf16),
            pltpu.VMEM((2, 16, LANES), f32),
            pltpu.VMEM((16, 2, LANES), f32),
            pltpu.VMEM((samples // LANES, LANES), f32),
            pltpu.VMEM((owners, 2, LANES), f32),
            pltpu.VMEM((det_size, 2, LANES), f32),
            dma((near_size - 1,)),
            dma((near_size - 1,)),
            dma((z_size - 1,)),
            dma((z_size - 1,)),
            dma((near_size - 1,)),
            dma((near_size - 1,)),
            dma((dets,)),
            dma((dets,)),
            dma,
            dma,
            dma((det_size - 1,)),
            dma((det_size - 1,)),
            dma,
        ],
        compiler_params=pltpu.CompilerParams(collective_id=0, has_side_effects=True, vmem_limit_bytes=67043328),
        name="whole",
    )(wafer_of, knee_freq, white_level, tile_order, data, templates, *stored)


def finish_kernel(
    flat_ref, amps_ref, own_ref, flat_out, amps_out, sky_out, weight_out, held, amps, own, sky, weight, come, go
):
    parts = come.shape[0] - 2
    rows = held.shape[0] // parts
    cuts = [pl.ds(k * rows, rows) for k in range(parts)]
    comes = [pltpu.make_async_copy(own_ref, own, come.at[parts]), pltpu.make_async_copy(amps_ref, amps, come.at[parts + 1])]
    comes += [pltpu.make_async_copy(flat_ref.at[cuts[k]], held.at[cuts[k]], come.at[k]) for k in range(parts)]
    goes = [pltpu.make_async_copy(held.at[cuts[k]], flat_out.at[cuts[k]], go.at[k]) for k in range(parts)]
    for copy in comes:
        copy.start()
    comes[0].wait()
    share = sky.shape[1]
    sky[...] = own[0:1, 0:share]
    weight[...] = own[1:2, 0:share]
    goes.append(pltpu.make_async_copy(sky, sky_out, go.at[parts]))
    goes.append(pltpu.make_async_copy(weight, weight_out, go.at[parts + 1]))
    for copy in goes[parts:]:
        copy.start()
    comes[1].wait()
    goes.append(pltpu.make_async_copy(amps, amps_out, go.at[parts + 2]))
    goes[-1].start()
    for k in range(parts):
        comes[2 + k].wait()
        goes[k].start()
    for copy in goes:
        copy.wait()


def finish(fit_amps, flat, own, share):
    hbm = pl.BlockSpec(memory_space=pltpu.HBM)
    parts = 4
    return pl.pallas_call(
        finish_kernel,
        out_shape=(
            jax.ShapeDtypeStruct(flat.shape, flat.dtype),
            jax.ShapeDtypeStruct(fit_amps.shape, fit_amps.dtype),
            jax.ShapeDtypeStruct((1, share), f32),
            jax.ShapeDtypeStruct((1, share), f32),
        ),
        in_specs=[hbm] * 3,
        out_specs=[hbm] * 4,
        scratch_shapes=[
            pltpu.VMEM(flat.shape, flat.dtype),
            pltpu.VMEM(fit_amps.shape, f32),
            pltpu.VMEM(own.shape, f32),
            pltpu.VMEM((1, share), f32),
            pltpu.VMEM((1, share), f32),
            pltpu.SemaphoreType.DMA((parts + 2,)),
            pltpu.SemaphoreType.DMA((parts + 3,)),
        ],
        compiler_params=pltpu.CompilerParams(vmem_limit_bytes=67043328),
        name="finish",
    )(flat, fit_amps, own)


def shards(mesh, *inputs):
    owners = mesh.shape["tm"]
    det_size = mesh.shape["det"]
    dets, samples = inputs[5].shape
    cells = 16 * PIX
    scale = float(cells) / float(dets * owners * det_size * samples)
    fit_amps, flat, maps = whole((owners // 16, 8, det_size), scale, owners, inputs)
    flat, fit_amps, sky, weight = finish(fit_amps, flat, maps, cells // owners)
    weighted = flat.reshape(samples // LANES, dets, LANES).transpose(1, 0, 2).reshape(dets, samples)
    return (fit_amps, weighted, sky.reshape(-1), weight.reshape(-1))


def solution(mesh):
    in_specs = (
        P("det", "tm"),
        P(None, None, "tm"),
        P("det"),
        P(("det", "tm")),
        P(("det", "tm")),
        P(("det", "tm"), None),
        P(("det", "tm"), None),
        P(),
    )
    out_specs = (P(None, "det"), P(("det", "tm"), None), P("tm"), P("tm"))
    return jax.shard_map(
        functools.partial(shards, mesh), mesh=mesh, in_specs=in_specs, out_specs=out_specs, check_vma=False
    )
```
